8 devices in a mesh: dp: 1 (over z), tp: 8 (over y, x, core).
Axes of the slice: x: 2, y: 2, z: 1, core: 2. Of those that a mesh axis runs over, the one named last changes fastest.
Arguments:
- tokens: bfloat16 [32, 64, 5120], P('dp')
- seq_lens: int32 [32], P('dp')
- w_q: bfloat16 [5120, 5120], P(None, 'tp')
- w_k: bfloat16 [5120, 1024], P(None, 'tp')
- w_v: bfloat16 [5120, 1024], P(None, 'tp')
- w_o: bfloat16 [5120, 5120], P('tp')
- g_q: bfloat16 [5120], P('tp')
- g_k: bfloat16 [1024], P('tp')
- g_attn: bfloat16 [5120], replicated
- g_mlp: bfloat16 [5120], replicated
- w_gate: bfloat16 [5120, 27648], P(None, 'tp')
- w_up: bfloat16 [5120, 27648], P(None, 'tp')
- w_down: bfloat16 [27648, 5120], P('tp')
Outputs:
- output 1: bfloat16 [32, 64, 5120], P('dp')
- output 2: bfloat16 [32, 8, 64, 128], P('dp', 'tp')
- output 3: bfloat16 [32, 8, 64, 128], P('dp', 'tp')
All inputs are finite; a program needn't handle non-finite values.
Results may differ from the reference program's by a relative error of at most 0.0157053.
Values are sent between devices in bfloat16 or wider.
A program may use at most 1 GiB of HBM per device.

```python
import jax
import jax.numpy as jnp
from jax import lax

PROMPTS = 32
SEQ_LEN = 64
D_MODEL = 5120
Q_HEADS = 40
KV_HEADS = 8
HEAD_DIM = 128
FF_DIM = 27648

ROPE_BASE = 500000.0
NORM_EPS = 1e-6


def setup_inputs(seed: int = 0, part: int = 0) -> dict:
    part_key = jax.random.fold_in(jax.random.key(seed), part)
    key_tok, key_len, key_slot = jax.random.split(part_key, 3)
    weight_keys = jax.random.split(jax.random.key(seed + 1), 13)
    q_width = Q_HEADS * HEAD_DIM
    kv_width = KV_HEADS * HEAD_DIM
    in_scale = D_MODEL ** -0.5
    tokens = jax.random.normal(key_tok, (PROMPTS, SEQ_LEN, D_MODEL), jnp.float32)
    seq_lens = jax.random.randint(key_len, (PROMPTS,), SEQ_LEN // 8, SEQ_LEN + 1, jnp.int32)
    full_slot = jax.random.randint(key_slot, (), 0, PROMPTS, jnp.int32)
    seq_lens = jnp.where(jnp.arange(PROMPTS) == full_slot, SEQ_LEN, seq_lens).astype(jnp.int32)
    q_head_scale = 2.0 ** jax.random.uniform(weight_keys[0], (Q_HEADS, 1), jnp.float32, -1.0, 1.0)
    k_head_scale = 2.0 ** jax.random.uniform(weight_keys[1], (KV_HEADS, 1), jnp.float32, -1.0, 1.0)
    w_q = (jax.random.normal(weight_keys[2], (D_MODEL, Q_HEADS, HEAD_DIM), jnp.float32) * q_head_scale * in_scale).reshape(D_MODEL, q_width)
    w_k = (jax.random.normal(weight_keys[3], (D_MODEL, KV_HEADS, HEAD_DIM), jnp.float32) * k_head_scale * in_scale).reshape(D_MODEL, kv_width)
    w_v = jax.random.normal(weight_keys[4], (D_MODEL, kv_width), jnp.float32) * in_scale
    w_o = jax.random.normal(weight_keys[5], (q_width, D_MODEL), jnp.float32) * q_width ** -0.5
    g_q = jax.random.uniform(weight_keys[6], (q_width,), jnp.float32, 0.5, 1.5)
    g_k = jax.random.uniform(weight_keys[7], (kv_width,), jnp.float32, 0.5, 1.5)
    g_attn = jax.random.uniform(weight_keys[8], (D_MODEL,), jnp.float32, 0.5, 1.5)
    g_mlp = jax.random.uniform(weight_keys[9], (D_MODEL,), jnp.float32, 0.5, 1.5)
    w_gate = jax.random.normal(weight_keys[10], (D_MODEL, FF_DIM), jnp.float32) * in_scale
    w_up = jax.random.normal(weight_keys[11], (D_MODEL, FF_DIM), jnp.float32) * in_scale
    w_down = jax.random.normal(weight_keys[12], (FF_DIM, D_MODEL), jnp.float32) * FF_DIM ** -0.5
    return dict(tokens=tokens.astype(jnp.bfloat16), seq_lens=seq_lens, w_q=w_q.astype(jnp.bfloat16), w_k=w_k.astype(jnp.bfloat16), w_v=w_v.astype(jnp.bfloat16), w_o=w_o.astype(jnp.bfloat16), g_q=g_q.astype(jnp.bfloat16), g_k=g_k.astype(jnp.bfloat16), g_attn=g_attn.astype(jnp.bfloat16), g_mlp=g_mlp.astype(jnp.bfloat16), w_gate=w_gate.astype(jnp.bfloat16), w_up=w_up.astype(jnp.bfloat16), w_down=w_down.astype(jnp.bfloat16))


def rope_tables(seq_len, head_dim):
    half_dim = head_dim // 2
    inv_freq = ROPE_BASE ** (-2.0 * jnp.arange(half_dim, dtype=jnp.float32) / head_dim)
    angles = jnp.arange(seq_len, dtype=jnp.float32)[:, None] * inv_freq[None, :]
    angles = jnp.concatenate([angles, angles], axis=-1)
    return jnp.cos(angles), jnp.sin(angles)


def apply_rope(vecs, cos_tab, sin_tab, head_axes):
    half_dim = vecs.shape[-1] // 2
    table_shape = (cos_tab.shape[0],) + (1,) * head_axes + (cos_tab.shape[1],)
    rotated = jnp.concatenate([-vecs[..., half_dim:], vecs[..., :half_dim]], axis=-1)
    return vecs * cos_tab.reshape(table_shape) + rotated * sin_tab.reshape(table_shape)


def rms_scale(vals):
    return lax.rsqrt(jnp.mean(vals * vals, axis=-1, keepdims=True) + NORM_EPS)


def post_norm(base, branch, gain):
    branch32 = branch.astype(jnp.float32)
    return (base.astype(jnp.float32) + branch32 * rms_scale(branch32) * gain.astype(jnp.float32)).astype(jnp.bfloat16)


def reference(tokens, seq_lens, w_q, w_k, w_v, w_o, g_q, g_k, g_attn, g_mlp, w_gate, w_up, w_down):
    group_size = Q_HEADS // KV_HEADS
    cos_tab, sin_tab = rope_tables(SEQ_LEN, HEAD_DIM)
    positions = jnp.arange(SEQ_LEN)
    causal = positions[None, :] <= positions[:, None]

    def one_prompt(item):
        prompt, length = item
        q_raw = jnp.dot(prompt, w_q, preferred_element_type=jnp.float32)
        k_raw = jnp.dot(prompt, w_k, preferred_element_type=jnp.float32)
        v_new = jnp.dot(prompt, w_v, preferred_element_type=jnp.float32).astype(jnp.bfloat16)
        q_norm = q_raw * rms_scale(q_raw) * g_q.astype(jnp.float32)
        k_norm = k_raw * rms_scale(k_raw) * g_k.astype(jnp.float32)
        queries = apply_rope(q_norm.reshape(SEQ_LEN, KV_HEADS, group_size, HEAD_DIM), cos_tab, sin_tab, 2).astype(jnp.bfloat16)
        keys_new = apply_rope(k_norm.reshape(SEQ_LEN, KV_HEADS, HEAD_DIM), cos_tab, sin_tab, 1).astype(jnp.bfloat16)
        v_heads = v_new.reshape(SEQ_LEN, KV_HEADS, HEAD_DIM)
        scores = jnp.einsum('sgrd,tgd->grst', queries.astype(jnp.float32), keys_new.astype(jnp.float32)) * HEAD_DIM ** -0.5
        allowed = causal & (positions[None, :] < length)
        scores = jnp.where(allowed, scores, -1e30)
        attn_probs = jax.nn.softmax(scores, axis=-1).astype(jnp.bfloat16)
        attn_out = jnp.einsum('grst,tgd->sgrd', attn_probs.astype(jnp.float32), v_heads.astype(jnp.float32)).astype(jnp.bfloat16)
        attn_proj = jnp.dot(attn_out.reshape(SEQ_LEN, Q_HEADS * HEAD_DIM), w_o, preferred_element_type=jnp.float32).astype(jnp.bfloat16)
        hidden = post_norm(prompt, attn_proj, g_attn)
        gate_pre = jnp.dot(hidden, w_gate, preferred_element_type=jnp.float32)
        up_proj = jnp.dot(hidden, w_up, preferred_element_type=jnp.float32)
        act_out = (jax.nn.silu(gate_pre) * up_proj).astype(jnp.bfloat16)
        mlp_out = jnp.dot(act_out, w_down, preferred_element_type=jnp.float32).astype(jnp.bfloat16)
        new_hidden = post_norm(hidden, mlp_out, g_mlp)
        return new_hidden, jnp.transpose(keys_new, (1, 0, 2)), jnp.transpose(v_heads, (1, 0, 2))

    out_hidden, k_cache, v_cache = lax.map(one_prompt, (tokens, seq_lens))
    return out_hidden, k_cache, v_cache
```

```python
import jax
import jax.numpy as jnp
from jax import lax
from jax.experimental import pallas as pl
from jax.experimental.pallas import tpu as pltpu
from jax.sharding import PartitionSpec as P

HEAD_DIM = 128
ROPE_BASE = 500000.0
NORM_EPS = 1e-6
CHUNKS = 4


def rope_tables(seq_len, head_dim):
    half_dim = head_dim // 2
    inv_freq = ROPE_BASE ** (-2.0 * jnp.arange(half_dim, dtype=jnp.float32) / head_dim)
    angles = jnp.arange(seq_len, dtype=jnp.float32)[:, None] * inv_freq[None, :]
    cos, sin = jnp.cos(angles), jnp.sin(angles)
    return jnp.concatenate([cos, cos], axis=-1), jnp.concatenate([-sin, sin], axis=-1)


def rms_scale(vals):
    return lax.rsqrt(jnp.mean(vals * vals, axis=-1, keepdims=True) + NORM_EPS)


def post_norm(base, branch, gain):
    branch32 = branch.astype(jnp.float32)
    return (base.astype(jnp.float32) + branch32 * rms_scale(branch32) * gain.astype(jnp.float32)).astype(jnp.bfloat16)


def attn_kernel(seq_len, group, per_step, lens_ref, q_ref, k_ref, v_ref, iq_ref, ik_ref, gq_ref, gk_ref, cos_ref, sin_ref, o_ref, kc_ref):
    step = pl.program_id(0)
    cos, sin = cos_ref[...], sin_ref[...]
    gk = gk_ref[...].astype(jnp.float32)

    def rope(t):
        return t * cos + pltpu.roll(t, HEAD_DIM // 2, 1) * sin

    row = lax.broadcasted_iota(jnp.int32, (seq_len, seq_len), 0)
    col = lax.broadcasted_iota(jnp.int32, (seq_len, seq_len), 1)
    for b in range(per_step):
        rows = pl.ds(b * seq_len, seq_len)
        keys = rope(k_ref[rows, :] * ik_ref[rows, :] * gk).astype(jnp.bfloat16)
        kc_ref[rows, :] = keys
        vals = v_ref[rows, :]
        inv_q = iq_ref[rows, :]
        qs = []
        for h in range(group):
            cols = pl.ds(h * HEAD_DIM, HEAD_DIM)
            qs.append(rope(q_ref[rows, cols] * inv_q * gq_ref[:, cols].astype(jnp.float32)).astype(jnp.bfloat16))
        queries = jnp.concatenate(qs, axis=0)
        scores = lax.dot_general(queries, keys, (((1,), (1,)), ((), ())), preferred_element_type=jnp.float32) * HEAD_DIM ** -0.5
        allowed = (col <= row) & (col < lens_ref[step * per_step + b])
        allowed = jnp.concatenate([allowed.astype(jnp.int32)] * group, axis=0) > 0
        scores = jnp.where(allowed, scores, -1e30)
        top = jnp.max(scores, axis=-1, keepdims=True)
        e = jnp.exp(scores - top)
        probs = (e / jnp.sum(e, axis=-1, keepdims=True)).astype(jnp.bfloat16)
        out = jnp.dot(probs, vals, preferred_element_type=jnp.float32).astype(jnp.bfloat16)
        for h in range(group):
            o_ref[rows, pl.ds(h * HEAD_DIM, HEAD_DIM)] = out[h * seq_len:(h + 1) * seq_len, :]


def attention(seq_lens, q_raw, k_raw, v, inv_q, inv_k, g_q, g_k, cos, sin, seq_len):
    tokens, width = q_raw.shape
    prompts = tokens // seq_len
    per_step = 4 if prompts % 4 == 0 else 1
    rows = per_step * seq_len
    group = width // HEAD_DIM
    def rs(w):
        return pl.BlockSpec((rows, w), lambda i, lens: (i, 0))
    def full(shape):
        return pl.BlockSpec(shape, lambda i, lens: (0, 0))
    import functools
    return pl.pallas_call(
        functools.partial(attn_kernel, seq_len, group, per_step),
        grid_spec=pltpu.PrefetchScalarGridSpec(
            num_scalar_prefetch=1,
            grid=(prompts // per_step,),
            in_specs=[rs(width), rs(HEAD_DIM), rs(HEAD_DIM), rs(1), rs(1), full((1, width)), full((1, HEAD_DIM)), full((seq_len, HEAD_DIM)), full((seq_len, HEAD_DIM))],
            out_specs=[rs(width), rs(HEAD_DIM)],
        ),
        out_shape=[jax.ShapeDtypeStruct((tokens, width), jnp.bfloat16), jax.ShapeDtypeStruct((tokens, HEAD_DIM), jnp.bfloat16)],
        cost_estimate=pl.CostEstimate(flops=4 * tokens * seq_len * width, bytes_accessed=tokens * width * 6, transcendentals=tokens * seq_len * group),
    )(seq_lens, q_raw, k_raw, v, inv_q, inv_k, g_q[None], g_k[None], cos, sin)


def solution(mesh):
    tp_size = mesh.shape['tp']

    def local_layer(tokens, seq_lens, w_q, w_k, w_v, w_o, g_q, g_k, g_attn, g_mlp, w_gate, w_up, w_down):
        prompts, seq_len, width = tokens.shape
        x = tokens.reshape(prompts * seq_len, width)
        me = lax.axis_index('tp')
        f32 = dict(preferred_element_type=jnp.float32)
        q_raw = jnp.dot(x, w_q, **f32)
        k_raw = jnp.dot(x, w_k, **f32)
        v = jnp.dot(x, w_v, **f32).astype(jnp.bfloat16)
        q_sumsq, k_sumsq = lax.psum((jnp.sum(q_raw * q_raw, axis=-1), jnp.sum(k_raw * k_raw, axis=-1)), 'tp')
        inv_q = lax.rsqrt(q_sumsq / (w_q.shape[1] * tp_size) + NORM_EPS)[:, None]
        inv_k = lax.rsqrt(k_sumsq / (w_k.shape[1] * tp_size) + NORM_EPS)[:, None]
        cos, sin = rope_tables(seq_len, HEAD_DIM)
        o, keys = attention(seq_lens, q_raw, k_raw, v, inv_q, inv_k, g_q, g_k, cos, sin, seq_len)
        k_cache = keys.reshape(prompts, 1, seq_len, HEAD_DIM)
        v_cache = v.reshape(prompts, 1, seq_len, HEAD_DIM)

        size = prompts * seq_len // CHUNKS
        own = size // tp_size
        outs = []
        hs = []
        for c in range(CHUNKS):
            part = jnp.dot(lax.slice_in_dim(o, c * size, (c + 1) * size), w_o, **f32).astype(jnp.bfloat16)
            a_own = lax.psum_scatter(part, 'tp', scatter_dimension=0, tiled=True)
            if hs:
                a_own, _ = lax.optimization_barrier((a_own, hs[-1][0]))
            x_own = lax.dynamic_slice_in_dim(x, c * size + me * own, own)
            h_own = post_norm(x_own, a_own, g_attn)
            hs.append((h_own, lax.all_gather(h_own, 'tp', axis=0, tiled=True)))
        for c in range(CHUNKS):
            h_own, h = hs[c]
            gate = jnp.dot(h, w_gate, **f32)
            up = jnp.dot(h, w_up, **f32)
            act = (jax.nn.silu(gate) * up).astype(jnp.bfloat16)
            part = jnp.dot(act, w_down, **f32).astype(jnp.bfloat16)
            m_own = lax.psum_scatter(part, 'tp', scatter_dimension=0, tiled=True)
            if outs:
                m_own, _ = lax.optimization_barrier((m_own, y_own))
            y_own = post_norm(h_own, m_own, g_mlp)
            outs.append(lax.all_gather(y_own, 'tp', axis=0, tiled=True))
        y = jnp.concatenate(outs, axis=0).reshape(prompts, seq_len, width)
        return y, k_cache, v_cache

    return jax.shard_map(local_layer, mesh=mesh, in_specs=(P('dp', None, None), P('dp'), P(None, 'tp'), P(None, 'tp'), P(None, 'tp'), P('tp', None), P('tp'), P('tp'), P(), P(), P(None, 'tp'), P(None, 'tp'), P('tp', None)), out_specs=(P('dp', None, None), P('dp', 'tp', None, None), P('dp', 'tp', None, None)), check_vma=False)
```

```python
import functools

import jax
import jax.numpy as jnp
from jax import lax
from jax.experimental import pallas as pl
from jax.experimental.pallas import tpu as pltpu
from jax.sharding import PartitionSpec as P

HEAD_DIM = 128
ROPE_BASE = 500000.0
NORM_EPS = 1e-6
CHUNKS = 4


def rope_tables(seq_len, head_dim):
    half_dim = head_dim // 2
    inv_freq = ROPE_BASE ** (-2.0 * jnp.arange(half_dim, dtype=jnp.float32) / head_dim)
    angles = jnp.arange(seq_len, dtype=jnp.float32)[:, None] * inv_freq[None, :]
    cos, sin = jnp.cos(angles), jnp.sin(angles)
    return jnp.concatenate([cos, cos], axis=-1), jnp.concatenate([-sin, sin], axis=-1)


def rms_scale(vals):
    return lax.rsqrt(jnp.mean(vals * vals, axis=-1, keepdims=True) + NORM_EPS)


def post_norm(base, branch, gain):
    branch32 = branch.astype(jnp.float32)
    return (base.astype(jnp.float32) + branch32 * rms_scale(branch32) * gain.astype(jnp.float32)).astype(jnp.bfloat16)


def attn_kernel(seq_len, group, per_step, lens_ref, q_ref, k_ref, v_ref, iq_ref, ik_ref, gq_ref, gk_ref, cos_ref, sin_ref, o_ref, kc_ref):
    step = pl.program_id(0)
    cos, sin = cos_ref[...], sin_ref[...]
    gk = gk_ref[...].astype(jnp.float32)

    def rope(t):
        return t * cos + pltpu.roll(t, HEAD_DIM // 2, 1) * sin

    row = lax.broadcasted_iota(jnp.int32, (seq_len, seq_len), 0)
    col = lax.broadcasted_iota(jnp.int32, (seq_len, seq_len), 1)
    for b in range(per_step):
        rows = pl.ds(b * seq_len, seq_len)
        keys = rope(k_ref[rows, :] * ik_ref[rows, :] * gk).astype(jnp.bfloat16)
        kc_ref[rows, :] = keys
        vals = v_ref[rows, :]
        inv_q = iq_ref[rows, :]
        qs = []
        for h in range(group):
            cols = pl.ds(h * HEAD_DIM, HEAD_DIM)
            qs.append(rope(q_ref[rows, cols] * inv_q * gq_ref[:, cols].astype(jnp.float32)).astype(jnp.bfloat16))
        queries = jnp.concatenate(qs, axis=0)
        scores = lax.dot_general(queries, keys, (((1,), (1,)), ((), ())), preferred_element_type=jnp.float32) * HEAD_DIM ** -0.5
        allowed = (col <= row) & (col < lens_ref[step * per_step + b])
        allowed = jnp.concatenate([allowed.astype(jnp.int32)] * group, axis=0) > 0
        scores = jnp.where(allowed, scores, -1e30)
        top = jnp.max(scores, axis=-1, keepdims=True)
        e = jnp.exp(scores - top)
        probs = (e / jnp.sum(e, axis=-1, keepdims=True)).astype(jnp.bfloat16)
        out = jnp.dot(probs, vals, preferred_element_type=jnp.float32).astype(jnp.bfloat16)
        for h in range(group):
            o_ref[rows, pl.ds(h * HEAD_DIM, HEAD_DIM)] = out[h * seq_len:(h + 1) * seq_len, :]


def attention(seq_lens, q_raw, k_raw, v, inv_q, inv_k, g_q, g_k, cos, sin, seq_len):
    tokens, width = q_raw.shape
    prompts = tokens // seq_len
    per_step = 4 if prompts % 4 == 0 else 1
    rows = per_step * seq_len
    group = width // HEAD_DIM
    def rs(w):
        return pl.BlockSpec((rows, w), lambda i, lens: (i, 0))
    def full(shape):
        return pl.BlockSpec(shape, lambda i, lens: (0, 0))
    return pl.pallas_call(
        functools.partial(attn_kernel, seq_len, group, per_step),
        grid_spec=pltpu.PrefetchScalarGridSpec(
            num_scalar_prefetch=1,
            grid=(prompts // per_step,),
            in_specs=[rs(width), rs(HEAD_DIM), rs(HEAD_DIM), rs(1), rs(1), full((1, width)), full((1, HEAD_DIM)), full((seq_len, HEAD_DIM)), full((seq_len, HEAD_DIM))],
            out_specs=[rs(width), rs(HEAD_DIM)],
        ),
        out_shape=[jax.ShapeDtypeStruct((tokens, width), jnp.bfloat16), jax.ShapeDtypeStruct((tokens, HEAD_DIM), jnp.bfloat16)],
        cost_estimate=pl.CostEstimate(flops=4 * tokens * seq_len * width, bytes_accessed=tokens * width * 6, transcendentals=tokens * seq_len * group),
    )(seq_lens, q_raw, k_raw, v, inv_q, inv_k, g_q[None], g_k[None], cos, sin)


MESH = pl.DeviceIdType.MESH
GU = 384
DN = 512
BLK = 16


def layer_kernel(chunks, x_ref, o_ref, wo_ref, wg_ref, wu_ref, wd_ref, ga_ref, gm_ref, y_ref,
                 wgu, wdb, wob, h, act, part, r0, r1, r2, obuf, xo, ho, yo,
                 gu_sem, wd_sem, wo_sem, o_sem, xo_sem, yo_sem, send, recv):
    size, width = part.shape
    gu_tiles = wg_ref.shape[1] // GU
    dn_tiles = width // DN
    steps = gu_tiles + dn_tiles
    me = lax.axis_index('tp')
    core = lax.rem(me, 2)
    xi = lax.rem(lax.div(me, 2), 2)
    yi = lax.div(me, 4)
    core_dev, x_dev, y_dev = me + 1 - 2 * core, me + 2 - 4 * xi, me + 4 - 8 * yi
    half = size // 2
    n0, n1, n2 = half // 2, half // 4, half // 8
    first, second = (xi, yi), (yi, xi)
    first_dev, second_dev = (x_dev, y_dev), (y_dev, x_dev)

    barrier = pltpu.get_barrier_semaphore()
    for dev in (core_dev, x_dev, y_dev):
        pl.semaphore_signal(barrier, inc=1, device_id={'tp': dev}, device_id_type=MESH)
    pl.semaphore_wait(barrier, 3)

    def rows(start, count):
        return pl.ds(pl.multiple_of(start, n2), count)

    def remote(stream, phase, col, chunk):
        base = col * half
        p = pl.multiple_of(base + core * n0, n0)
        q = pl.multiple_of(p + first[col] * n1, n1)
        own = pl.multiple_of(q + second[col] * n2, n2)
        if phase == 0:
            src, dst, dev = part.at[rows(base + (1 - core) * n0, n0)], r0.at[stream, pl.ds(col * n0, n0)], core_dev
        elif phase == 1:
            src, dst, dev = r0.at[stream, rows(col * n0 + (1 - first[col]) * n1, n1)], r1.at[stream, pl.ds(col * n1, n1)], first_dev[col]
        elif phase == 2:
            src, dst, dev = r1.at[stream, rows(col * n1 + (1 - second[col]) * n2, n2)], r2.at[stream, pl.ds(col * n2, n2)], second_dev[col]
        else:
            start, count, dev = ((own, n2, second_dev[col]), (q, n1, first_dev[col]), (p, n0, core_dev))[phase - 3]
            if stream == 0:
                src = dst = h.at[lax.rem(chunk, 2), rows(start, count)]
            else:
                dst = y_ref.at[rows(chunk * size + start, count)]
                src = yo.at[pl.ds(col * n2, n2)] if phase == 3 else dst
        return pltpu.make_async_remote_copy(src_ref=src, dst_ref=dst, send_sem=send.at[stream, phase, col], recv_sem=recv.at[stream, phase, col], device_id={'tp': dev}, device_id_type=MESH)

    def own_row(col):
        return col * half + core * n0 + first[col] * n1 + second[col] * n2

    def x_copy(col, chunk):
        return pltpu.make_async_copy(x_ref.at[rows(chunk * size + own_row(col), n2)], xo.at[pl.ds(col * n2, n2)], xo_sem.at[col])

    def y_copy(col, chunk):
        return pltpu.make_async_copy(yo.at[pl.ds(col * n2, n2)], y_ref.at[rows(chunk * size + own_row(col), n2)], yo_sem.at[col])

    def o_copy(chunk):
        return pltpu.make_async_copy(o_ref.at[rows(chunk * size, size)], obuf, o_sem)

    def gu_copies(chunk, j):
        slot = lax.rem(chunk * gu_tiles + j, 2)
        cols = pl.ds(pl.multiple_of(j * GU, GU), GU)
        return (pltpu.make_async_copy(wg_ref.at[:, cols], wgu.at[slot, :, pl.ds(0, GU)], gu_sem.at[slot, 0]),
                pltpu.make_async_copy(wu_ref.at[:, cols], wgu.at[slot, :, pl.ds(GU, GU)], gu_sem.at[slot, 1]))

    def dn_copy(k):
        slot = lax.rem(k, 2)
        return pltpu.make_async_copy(wd_ref.at[:, pl.ds(pl.multiple_of(k * DN, DN), DN)], wdb.at[slot], wd_sem.at[slot])

    def add_into(dst, dst_start, src, src_start, count):
        @pl.loop(0, count // BLK)
        def _(i):
            d = pl.ds(pl.multiple_of(dst_start + i * BLK, BLK), BLK)
            s = pl.ds(pl.multiple_of(src_start + i * BLK, BLK), BLK)
            dst[d, :] = (dst[d, :].astype(jnp.float32) + src[s, :].astype(jnp.float32)).astype(jnp.bfloat16)

    def project(chunk):
        o_copy(chunk).wait()

        @pl.loop(0, dn_tiles)
        def _(k):
            cols = pl.ds(pl.multiple_of(k * DN, DN), DN)
            part[:, cols] = jnp.dot(obuf[...], wob[:, cols], preferred_element_type=jnp.float32).astype(jnp.bfloat16)

    def event(stream, e, chunk):
        for col in range(2):
            if e == 0:
                remote(stream, 0, col, chunk).start()
                continue
            prev = remote(stream, e - 1, col, chunk)
            prev.wait_recv()
            prev.wait_send()
            if e == 1:
                add_into(r0.at[stream], col * n0, part, col * half + core * n0, n0)
            elif e == 2:
                add_into(r1.at[stream], col * n1, r0.at[stream], col * n0 + first[col] * n1, n1)
                if stream == 0:
                    x_copy(col, chunk).start()
            elif e == 3:
                gain = ga_ref if stream == 0 else gm_ref
                par = lax.rem(chunk, 2)
                if stream == 0:
                    x_copy(col, chunk).wait()

                @pl.loop(0, n2 // BLK)
                def _(i):
                    mine = pl.ds(pl.multiple_of(col * n2 + i * BLK, BLK), BLK)
                    kept = pl.ds(pl.multiple_of(col * n1 + second[col] * n2 + i * BLK, BLK), BLK)
                    total = (r2[stream, mine, :].astype(jnp.float32) + r1[stream, kept, :].astype(jnp.float32)).astype(jnp.bfloat16)
                    base = xo[mine, :] if stream == 0 else ho[par, mine, :]
                    out = post_norm(base, total, gain[...])
                    if stream == 0:
                        h[par, pl.ds(pl.multiple_of(own_row(col) + i * BLK, BLK), BLK), :] = out
                        ho[par, mine, :] = out
                    else:
                        yo[mine, :] = out
                if stream == 1:
                    y_copy(col, chunk).start()
            elif e == 4 and stream == 1:
                y_copy(col, chunk).wait()
            if e < 6:
                remote(stream, e, col, chunk).start()

    pltpu.make_async_copy(wo_ref, wob, wo_sem).start()
    o_copy(0).start()
    for cp in gu_copies(0, 0):
        cp.start()
    dn_copy(0).start()
    pltpu.make_async_copy(wo_ref, wob, wo_sem).wait()

    points = {(1, 1): 1, (1, 2): 4, (1, 3): 6, (1, 4): 8, (1, 5): 11, (1, 6): 15,
              (0, 0): 1, (0, 1): 2, (0, 2): 5, (0, 3): 7, (0, 4): 10, (0, 5): 14, (0, 6): 18}

    @pl.loop(0, chunks + 2)
    def _(it):
        c = it - 1
        computes = (it >= 1) & (it <= chunks)

        @pl.loop(0, steps)
        def _(j):
            for (stream, e), at in sorted(points.items(), key=lambda kv: (kv[1], -kv[0][0])):
                live = (it < chunks) if stream == 0 else (it >= 2)

                @pl.when((j == at) & live)
                def _():
                    chunk = it if stream == 0 else it - 2
                    if (stream, e) == (0, 0):
                        project(chunk)

                        @pl.when(it + 1 < chunks)
                        def _():
                            o_copy(chunk + 1).start()
                    event(stream, e, chunk)

            @pl.when(computes & (j < gu_tiles))
            def _():
                for cp in gu_copies(c, j):
                    cp.wait()

                @pl.when((j + 1 < gu_tiles) | (it < chunks))
                def _():
                    wraps = (j + 1 >= gu_tiles).astype(jnp.int32)
                    for cp in gu_copies(c + wraps, (j + 1) * (1 - wraps)):
                        cp.start()
                slot = lax.rem(c * gu_tiles + j, 2)
                both = jnp.dot(h[lax.rem(c, 2)], wgu[slot], preferred_element_type=jnp.float32)
                gate, up = both[:, :GU], both[:, GU:]
                act[:, pl.ds(pl.multiple_of(j * GU, GU), GU)] = (gate * lax.logistic(gate) * up).astype(jnp.bfloat16)

            @pl.when(computes & (j >= gu_tiles))
            def _():
                k = j - gu_tiles
                dn_copy(k).wait()

                @pl.when((k + 1 < dn_tiles) | (it < chunks))
                def _():
                    wraps = (k + 1 >= dn_tiles).astype(jnp.int32)
                    dn_copy((k + 1) * (1 - wraps)).start()
                part[:, pl.ds(pl.multiple_of(k * DN, DN), DN)] = jnp.dot(act[...], wdb[lax.rem(k, 2)], preferred_element_type=jnp.float32).astype(jnp.bfloat16)

        @pl.when(computes)
        def _():
            event(1, 0, c)


def layer_tail(x, o, w_o, w_gate, w_up, w_down, g_attn, g_mlp):
    tokens, width = x.shape
    size = tokens // CHUNKS
    inner = w_gate.shape[1]
    bf = jnp.bfloat16
    anyspec = pl.BlockSpec(memory_space=pl.ANY)
    vmem = pl.BlockSpec(memory_space=pltpu.VMEM)
    dma = pltpu.SemaphoreType.DMA
    return pl.pallas_call(
        functools.partial(layer_kernel, CHUNKS),
        out_shape=jax.ShapeDtypeStruct((tokens, width), bf),
        in_specs=[anyspec] * 6 + [vmem] * 2,
        out_specs=anyspec,
        scratch_shapes=[
            pltpu.VMEM((2, width, 2 * GU), bf), pltpu.VMEM((2, inner, DN), bf), pltpu.VMEM(w_o.shape, bf),
            pltpu.VMEM((2, size, width), bf), pltpu.VMEM((size, inner), bf), pltpu.VMEM((size, width), bf),
            pltpu.VMEM((2, size // 2, width), bf), pltpu.VMEM((2, size // 4, width), bf), pltpu.VMEM((2, size // 8, width), bf),
            pltpu.VMEM((size, o.shape[1]), bf), pltpu.VMEM((size // 8, width), bf), pltpu.VMEM((2, size // 8, width), bf), pltpu.VMEM((size // 8, width), bf),
            dma((2, 2)), dma((2,)), dma, dma, dma((2,)), dma((2,)), dma((2, 6, 2)), dma((2, 6, 2)),
        ],
        compiler_params=pltpu.CompilerParams(collective_id=0, has_side_effects=True, vmem_limit_bytes=67043328),
        cost_estimate=pl.CostEstimate(flops=2 * tokens * width * (3 * inner + o.shape[1]), bytes_accessed=CHUNKS * 3 * inner * width * 2, transcendentals=tokens * inner),
    )(x, o, w_o, w_gate, w_up, w_down, g_attn[None], g_mlp[None])


def solution(mesh):
    tp_size = mesh.shape['tp']

    def local_layer(tokens, seq_lens, w_q, w_k, w_v, w_o, g_q, g_k, g_attn, g_mlp, w_gate, w_up, w_down):
        prompts, seq_len, width = tokens.shape
        x = tokens.reshape(prompts * seq_len, width)
        f32 = dict(preferred_element_type=jnp.float32)
        q_raw = jnp.dot(x, w_q, **f32)
        k_raw = jnp.dot(x, w_k, **f32)
        v = jnp.dot(x, w_v, **f32).astype(jnp.bfloat16)
        q_sumsq, k_sumsq = lax.psum((jnp.sum(q_raw * q_raw, axis=-1), jnp.sum(k_raw * k_raw, axis=-1)), 'tp')
        inv_q = lax.rsqrt(q_sumsq / (w_q.shape[1] * tp_size) + NORM_EPS)[:, None]
        inv_k = lax.rsqrt(k_sumsq / (w_k.shape[1] * tp_size) + NORM_EPS)[:, None]
        cos, sin = rope_tables(seq_len, HEAD_DIM)
        o, keys = attention(seq_lens, q_raw, k_raw, v, inv_q, inv_k, g_q, g_k, cos, sin, seq_len)
        k_cache = keys.reshape(prompts, 1, seq_len, HEAD_DIM)
        v_cache = v.reshape(prompts, 1, seq_len, HEAD_DIM)

        y = layer_tail(x, o, w_o, w_gate, w_up, w_down, g_attn, g_mlp).reshape(prompts, seq_len, width)
        return y, k_cache, v_cache

    return jax.shard_map(local_layer, mesh=mesh, in_specs=(P('dp', None, None), P('dp'), P(None, 'tp'), P(None, 'tp'), P(None, 'tp'), P('tp', None), P('tp'), P('tp'), P(), P(), P(None, 'tp'), P(None, 'tp'), P('tp', None)), out_specs=(P('dp', None, None), P('dp', 'tp', None, None), P('dp', 'tp', None, None)), check_vma=False)
```

```python
import functools

import jax
import jax.numpy as jnp
import numpy as np
from jax import lax
from jax.experimental import pallas as pl
from jax.experimental.pallas import tpu as pltpu
from jax.sharding import PartitionSpec as P

HEAD_DIM = 128
ROPE_BASE = 500000.0
NORM_EPS = 1e-6
MESH = pl.DeviceIdType.MESH
CHUNKS = 4
GU = 384
DN = 512
BLK = 16
STAT = 128

PROLOGUE, STEPS = 19, 103
EVENTS = {
    (2, 0): (0, 3, 6, 13),
    (2, 1): (1, 5, 11, 16),
    (0, 6): (18, 29, 43, 60),
    (0, 5): (17, 27, 41, 59),
    (0, 4): (12, 22, 32, 51),
    (0, 3): (9, 20, 28, 47),
    (0, 2): (7, 14, 25, 38),
    (0, 1): (4, 10, 20, 28),
    (0, 0): (2, 8, 15, 25),
    (1, 6): (64, 79, 97, 102),
    (1, 5): (62, 78, 95, 101),
    (1, 4): (54, 71, 87, 100),
    (1, 3): (47, 66, 84, 99),
    (1, 2): (45, 64, 82, 98),
    (1, 1): (39, 59, 78, 96),
}


def rope_tables(seq_len, head_dim):
    half_dim = head_dim // 2
    inv_freq = np.float32(ROPE_BASE) ** (np.float32(-2.0) * np.arange(half_dim, dtype=np.float32) / np.float32(head_dim))
    angles = np.arange(seq_len, dtype=np.float32)[:, None] * inv_freq[None, :].astype(np.float32)
    cos, sin = np.cos(angles).astype(np.float32), np.sin(angles).astype(np.float32)
    return np.concatenate([cos, cos], axis=-1), np.concatenate([-sin, sin], axis=-1)


def rms_scale(vals):
    return lax.rsqrt(jnp.mean(vals * vals, axis=-1, keepdims=True) + NORM_EPS)


def post_norm(base, branch, gain):
    branch32 = branch.astype(jnp.float32)
    return (base.astype(jnp.float32) + branch32 * rms_scale(branch32) * gain.astype(jnp.float32)).astype(jnp.bfloat16)


def layer_kernel(seq_len, tp_size, lens_ref, x_ref, wq_ref, wk_ref, wv_ref, wo_ref, wg_ref, wu_ref, wd_ref,
                 gq_ref, gk_ref, ga_ref, gm_ref, cos_ref, sin_ref, y_ref, kc_ref, vc_ref,
                 wgu, wdb, h, act, part, r0, r1, r2, obuf, qk, ho, yo, stat, stat_in, inv,
                 gu_sem, wd_sem, wo_sem, wqkv_sem, x_sem, ho_sem, yo_sem, st_send, st_recv, send, recv, free, hfree):
    size, width = part.shape
    q_width = obuf.shape[1]
    group = q_width // HEAD_DIM
    gu_tiles = wg_ref.shape[1] // GU
    dn_tiles = width // DN
    per_slot = dn_tiles // 2
    per_chunk = gu_tiles + dn_tiles
    me = lax.axis_index('tp')
    core = lax.rem(me, 2)
    xi = lax.rem(lax.div(me, 2), 2)
    yi = lax.div(me, 4)
    partners = (me + 1 - 2 * core, me + 2 - 4 * xi, me + 4 - 8 * yi)
    core_dev = partners[0]
    parts = 4
    quarter = size // parts
    n0, n1, n2 = quarter // 2, quarter // 4, quarter // 8
    first, second = (xi, yi), (yi, xi)
    first_dev, second_dev = partners[1:], partners[:0:-1]

    barrier = pltpu.get_barrier_semaphore()
    for r in range(1, tp_size):
        pl.semaphore_signal(barrier, inc=1, device_id={'tp': lax.rem(me + r, tp_size)}, device_id_type=MESH)

    def rows(start, count):
        return pl.ds(pl.multiple_of(start, BLK), count)

    def remote(stream, phase, p, chunk):
        col = p % 2
        a = p * quarter + core * n0
        b = a + first[col] * n1
        own = b + second[col] * n2
        if phase == 0:
            src, dst, dev = part.at[rows(p * quarter + (1 - core) * n0, n0)], r0.at[stream, pl.ds(p * n0, n0)], core_dev
        elif phase == 1:
            src, dst, dev = r0.at[stream, rows(p * n0 + (1 - first[col]) * n1, n1)], r1.at[stream, pl.ds(p * n1, n1)], first_dev[col]
        elif phase == 2:
            src, dst, dev = r1.at[stream, rows(p * n1 + (1 - second[col]) * n2, n2)], r2.at[stream, pl.ds(p * n2, n2)], second_dev[col]
        else:
            start, count, dev = ((own, n2, second_dev[col]), (b, n1, first_dev[col]), (a, n0, core_dev))[phase - 3]
            if stream == 0:
                src = dst = h.at[lax.rem(chunk, 2), rows(start, count)]
            else:
                dst = y_ref.at[rows(chunk * size + start, count)]
                src = yo.at[pl.ds(p * n2, n2)] if phase == 3 else dst
        return pltpu.make_async_remote_copy(src_ref=src, dst_ref=dst, send_sem=send.at[stream, chunk, phase, p], recv_sem=recv.at[stream, chunk, phase, p], device_id={'tp': dev}, device_id_type=MESH)

    def own_row(p):
        return p * quarter + core * n0 + first[p % 2] * n1 + second[p % 2] * n2

    def base_copy(p, chunk):
        return pltpu.make_async_copy(x_ref.at[rows(chunk * size + own_row(p), n2)], ho.at[chunk, pl.ds(p * n2, n2)], ho_sem.at[chunk, p])

    def y_copy(p, chunk):
        return pltpu.make_async_copy(yo.at[pl.ds(p * n2, n2)], y_ref.at[rows(chunk * size + own_row(p), n2)], yo_sem.at[p])

    def x_copy(chunk):
        return pltpu.make_async_copy(x_ref.at[rows(chunk * size, size)], h.at[1], x_sem)

    def wo_copies():
        return [pltpu.make_async_copy(wo_ref.at[:, pl.ds(k * DN, DN)], wdb.at[k // per_slot, pl.ds(k % per_slot * q_width, q_width)], wo_sem.at[k]) for k in range(dn_tiles)]

    def qkv_copies():
        return (pltpu.make_async_copy(wq_ref, wgu.at[0, :, pl.ds(0, q_width)], wqkv_sem.at[0]),
                pltpu.make_async_copy(wk_ref, wgu.at[0, :, pl.ds(q_width, HEAD_DIM)], wqkv_sem.at[1]),
                pltpu.make_async_copy(wv_ref, wgu.at[1, :, pl.ds(0, HEAD_DIM)], wqkv_sem.at[2]))

    def gu_copies(chunk, j):
        slot = lax.rem(chunk * gu_tiles + j, 2)
        cols = pl.ds(pl.multiple_of(j * GU, GU), GU)
        return (pltpu.make_async_copy(wg_ref.at[:, cols], wgu.at[slot, :, pl.ds(0, GU)], gu_sem.at[slot, 0]),
                pltpu.make_async_copy(wu_ref.at[:, cols], wgu.at[slot, :, pl.ds(GU, GU)], gu_sem.at[slot, 1]))

    def dn_copy(k):
        slot = lax.rem(k, 2)
        return pltpu.make_async_copy(wd_ref.at[:, pl.ds(pl.multiple_of(k * DN, DN), DN)], wdb.at[slot], wd_sem.at[slot])

    def stat_copy(r, chunk):
        return pltpu.make_async_remote_copy(src_ref=stat.at[chunk], dst_ref=stat_in.at[chunk, r - 1], send_sem=st_send.at[chunk, r - 1], recv_sem=st_recv.at[chunk, r - 1], device_id={'tp': lax.rem(me + r, tp_size)}, device_id_type=MESH)

    def release_h():
        for i, dev in enumerate(partners):
            pl.semaphore_signal(hfree.at[i], inc=1, device_id={'tp': dev}, device_id_type=MESH)

    def add_into(dst, dst_start, src, src_start, count):
        @pl.loop(0, count // BLK)
        def _(i):
            d = pl.ds(pl.multiple_of(dst_start + i * BLK, BLK), BLK)
            s = pl.ds(pl.multiple_of(src_start + i * BLK, BLK), BLK)
            dst[d, :] = (dst[d, :].astype(jnp.float32) + src[s, :].astype(jnp.float32)).astype(jnp.bfloat16)

    def project_qkv(chunk):
        @pl.when(chunk == 0)
        def _():
            for cp in qkv_copies():
                cp.wait()
        x_copy(chunk).wait()
        qk[...] = jnp.dot(h[1], wgu[0], preferred_element_type=jnp.float32)
        vc_ref[rows(chunk * size, size), :] = jnp.dot(h[1], wgu[1, :, pl.ds(0, HEAD_DIM)], preferred_element_type=jnp.float32).astype(jnp.bfloat16)

        @pl.when(chunk + 1 < CHUNKS)
        def _():
            x_copy(chunk + 1).start()

        @pl.when(chunk + 1 == CHUNKS)
        def _():
            release_h()
            for cp in gu_copies(0, 0):
                cp.start()
        sums = []
        for blk in range(size // STAT):
            r = pl.ds(blk * STAT, STAT)
            squares = [jnp.square(qk[r, pl.ds(t * HEAD_DIM, HEAD_DIM)]) for t in range(group + 1)]
            for sq in (sum(squares[1:group], squares[0]), squares[group]):
                sums.append(jnp.sum(sq.T, axis=0, keepdims=True))
        stat[chunk] = jnp.concatenate(sums, axis=0)
        for r in range(1, tp_size):
            stat_copy(r, chunk).start()

    def attend(chunk):
        total = stat[chunk]
        for r in range(1, tp_size):
            stat_copy(r, chunk).wait()
        for r in range(1, tp_size):
            total = total + stat_in[chunk, r - 1]
        inv[0] = lax.rsqrt(total / (q_width * tp_size) + NORM_EPS)
        inv[1] = lax.rsqrt(total / (HEAD_DIM * tp_size) + NORM_EPS)
        cos, sin = cos_ref[...], sin_ref[...]
        gk = gk_ref[...].astype(jnp.float32)
        row = lax.broadcasted_iota(jnp.int32, (seq_len, seq_len), 0)
        col = lax.broadcasted_iota(jnp.int32, (seq_len, seq_len), 1)

        def rope(t):
            return t * cos + pltpu.roll(t, HEAD_DIM // 2, 1) * sin

        @pl.loop(0, size // STAT)
        def _(blk):
            iq = jnp.broadcast_to(inv[0, pl.ds(2 * blk, 1), :], (STAT, HEAD_DIM)).T
            ik = jnp.broadcast_to(inv[1, pl.ds(2 * blk + 1, 1), :], (STAT, HEAD_DIM)).T
            for b in range(STAT // seq_len):
                local = pl.ds(pl.multiple_of(blk * STAT + b * seq_len, seq_len), seq_len)
                mine = pl.ds(pl.multiple_of(chunk * size + blk * STAT + b * seq_len, seq_len), seq_len)
                inv_q, inv_k = iq[b * seq_len:(b + 1) * seq_len, :], ik[b * seq_len:(b + 1) * seq_len, :]
                keys = rope(qk[local, pl.ds(q_width, HEAD_DIM)] * inv_k * gk).astype(jnp.bfloat16)
                kc_ref[mine, :] = keys
                qs = []
                for hd in range(group):
                    cols = pl.ds(hd * HEAD_DIM, HEAD_DIM)
                    qs.append(rope(qk[local, cols] * inv_q * gq_ref[:, cols].astype(jnp.float32)).astype(jnp.bfloat16))
                queries = jnp.concatenate(qs, axis=0)
                scores = lax.dot_general(queries, keys, (((1,), (1,)), ((), ())), preferred_element_type=jnp.float32) * HEAD_DIM ** -0.5
                length = lens_ref[chunk * (size // seq_len) + blk * (STAT // seq_len) + b]
                allowed = ((col <= row) & (col < length)).astype(jnp.int32)
                scores = jnp.where(jnp.concatenate([allowed] * group, axis=0) > 0, scores, -1e30)
                e = jnp.exp(scores - jnp.max(scores, axis=-1, keepdims=True))
                probs = (e / jnp.sum(e, axis=-1, keepdims=True)).astype(jnp.bfloat16)
                out = jnp.dot(probs, vc_ref[mine, :], preferred_element_type=jnp.float32).astype(jnp.bfloat16)
                for hd in range(group):
                    obuf[mine, pl.ds(hd * HEAD_DIM, HEAD_DIM)] = out[hd * seq_len:(hd + 1) * seq_len, :]

    def project(chunk):
        @pl.when(chunk == 0)
        def _():
            for cp in wo_copies():
                cp.wait()

        @pl.loop(0, dn_tiles)
        def _(k):
            w = wdb[lax.div(k, per_slot), pl.ds(pl.multiple_of(lax.rem(k, per_slot) * q_width, q_width), q_width), :]
            cols = pl.ds(pl.multiple_of(k * DN, DN), DN)
            part[:, cols] = jnp.dot(obuf[rows(chunk * size, size), :], w, preferred_element_type=jnp.float32).astype(jnp.bfloat16)

    def take(sem, chunk):
        @pl.when(chunk >= 1)
        def _():
            pl.semaphore_wait(sem, 1)

    def give(sem, chunk, dev):
        @pl.when(chunk + 1 < CHUNKS)
        def _():
            pl.semaphore_signal(sem, inc=1, device_id={'tp': dev}, device_id_type=MESH)

    def event(stream, e, chunk):
        for p in range(parts):
            col = p % 2
            if e > 0:
                prev = remote(stream, e - 1, p, chunk)
                prev.wait_recv()
                prev.wait_send()
            if e == 1:
                add_into(r0.at[stream], p * n0, part, p * quarter + core * n0, n0)
            elif e == 2:
                add_into(r1.at[stream], p * n1, r0.at[stream], p * n0 + first[col] * n1, n1)
                give(free.at[stream, 0, p], chunk, core_dev)
            elif e == 3:
                gain = ga_ref if stream == 0 else gm_ref
                mine = pl.ds(p * n2, n2)
                kept = rows(p * n1 + second[col] * n2, n2)
                total = (r2[stream, mine, :].astype(jnp.float32) + r1[stream, kept, :].astype(jnp.float32)).astype(jnp.bfloat16)
                if stream == 0:
                    base_copy(p, chunk).wait()
                out = post_norm(ho[chunk, mine, :], total, gain[...])
                if stream == 0:
                    if p == 0:
                        for i in range(len(partners)):
                            take(hfree.at[i], chunk)
                    h[lax.rem(chunk, 2), rows(own_row(p), n2), :] = out
                    ho[chunk, mine, :] = out
                else:
                    yo[mine, :] = out
                    y_copy(p, chunk).start()
                give(free.at[stream, 1, p], chunk, first_dev[col])
                give(free.at[stream, 2, p], chunk, second_dev[col])
            elif e == 4 and stream == 1:
                y_copy(p, chunk).wait()
            if e < 3:
                take(free.at[stream, e, p], chunk)
            if e < 6:
                remote(stream, e, p, chunk).start()

    for cp in qkv_copies():
        cp.start()
    x_copy(0).start()
    for cp in wo_copies():
        cp.start()
    for chunk in range(CHUNKS):
        for p in range(parts):
            base_copy(p, chunk).start()
    pl.semaphore_wait(barrier, tp_size - 1)

    reload_wo = sorted({(s - PROLOGUE) // per_chunk for s in EVENTS[0, 0] if s >= PROLOGUE} - {0})

    @pl.loop(0, STEPS)
    def _(g):
        gm = g - PROLOGUE
        c, j = lax.div(gm, per_chunk), lax.rem(gm, per_chunk)
        computes = (gm >= 0) & (gm < CHUNKS * per_chunk)

        for it in reload_wo:
            @pl.when(gm == it * per_chunk + 1)
            def _():
                for cp in wo_copies():
                    cp.wait()

        for (stream, e), at in EVENTS.items():
            hit = functools.reduce(lambda a, b: a | b, [g == s for s in at])

            @pl.when(hit)
            def _():
                chunk = sum([(g >= s).astype(jnp.int32) for s in at[1:]])
                if stream == 2:
                    (project_qkv, attend)[e](chunk)
                else:
                    if (stream, e) == (0, 0):
                        project(chunk)
                    event(stream, e, chunk)

        @pl.when(computes & (j < gu_tiles))
        def _():
            for cp in gu_copies(c, j):
                cp.wait()

            @pl.when((j + 1 < gu_tiles) | (c + 1 < CHUNKS))
            def _():
                wraps = (j + 1 >= gu_tiles).astype(jnp.int32)
                for cp in gu_copies(c + wraps, (j + 1) * (1 - wraps)):
                    cp.start()

            @pl.when(j == gu_tiles - 2)
            def _():
                dn_copy(0).start()
            slot = lax.rem(c * gu_tiles + j, 2)
            both = jnp.dot(h[lax.rem(c, 2)], wgu[slot], preferred_element_type=jnp.float32)
            gate, up = both[:, :GU], both[:, GU:]
            act[:, pl.ds(pl.multiple_of(j * GU, GU), GU)] = (gate * lax.logistic(gate) * up).astype(jnp.bfloat16)

            @pl.when((j == gu_tiles - 1) & (c + 2 < CHUNKS))
            def _():
                release_h()

        @pl.when(computes & (j >= gu_tiles))
        def _():
            k = j - gu_tiles
            dn_copy(k).wait()

            @pl.when(k + 1 < dn_tiles)
            def _():
                dn_copy(k + 1).start()
            part[:, pl.ds(pl.multiple_of(k * DN, DN), DN)] = jnp.dot(act[...], wdb[lax.rem(k, 2)], preferred_element_type=jnp.float32).astype(jnp.bfloat16)

            @pl.when(k + 1 == dn_tiles)
            def _():
                event(1, 0, c)
            for it in reload_wo:
                @pl.when(gm == it * per_chunk - 1)
                def _():
                    for cp in wo_copies():
                        cp.start()


def solution(mesh):
    tp_size = mesh.shape['tp']

    def local_layer(tokens, seq_lens, w_q, w_k, w_v, w_o, g_q, g_k, g_attn, g_mlp, w_gate, w_up, w_down):
        prompts, seq_len, width = tokens.shape
        total, inner, q_width = prompts * seq_len, w_gate.shape[1], w_q.shape[1]
        size = total // CHUNKS
        cos, sin = rope_tables(seq_len, HEAD_DIM)
        bf, f32 = jnp.bfloat16, jnp.float32
        anyspec = pl.BlockSpec(memory_space=pl.ANY)
        vmem = pl.BlockSpec(memory_space=pltpu.VMEM)
        dma, credit = pltpu.SemaphoreType.DMA, pltpu.SemaphoreType.REGULAR
        kv = jax.ShapeDtypeStruct((total, HEAD_DIM), bf)
        y, keys, v = pl.pallas_call(
            functools.partial(layer_kernel, seq_len, tp_size),
            out_shape=[jax.ShapeDtypeStruct((total, width), bf), kv, kv],
            in_specs=[pl.BlockSpec(memory_space=pltpu.SMEM)] + [anyspec] * 8 + [vmem] * 6,
            out_specs=[anyspec, vmem, vmem],
            scratch_shapes=[
                pltpu.VMEM((2, width, 2 * GU), bf), pltpu.VMEM((2, inner, DN), bf), pltpu.VMEM((2, size, width), bf),
                pltpu.VMEM((size, inner), bf), pltpu.VMEM((size, width), bf),
                pltpu.VMEM((2, size // 2, width), bf), pltpu.VMEM((2, size // 4, width), bf), pltpu.VMEM((2, size // 8, width), bf),
                pltpu.VMEM((total, q_width), bf), pltpu.VMEM((size, q_width + HEAD_DIM), f32),
                pltpu.VMEM((CHUNKS, size // 8, width), bf), pltpu.VMEM((size // 8, width), bf),
                pltpu.VMEM((CHUNKS, 8, STAT), f32), pltpu.VMEM((CHUNKS, tp_size - 1, 8, STAT), f32), pltpu.VMEM((2, 8, STAT), f32),
                dma((2, 2)), dma((2,)), dma((width // DN,)), dma((3,)), dma, dma((CHUNKS, 4)), dma((4,)),
                dma((CHUNKS, tp_size - 1)), dma((CHUNKS, tp_size - 1)), dma((2, CHUNKS, 6, 4)), dma((2, CHUNKS, 6, 4)),
                credit((2, 3, 4)), credit((3,)),
            ],
            compiler_params=pltpu.CompilerParams(collective_id=0, has_side_effects=True, vmem_limit_bytes=67043328),
            cost_estimate=pl.CostEstimate(flops=2 * total * width * (3 * inner + 2 * q_width + 2 * HEAD_DIM), bytes_accessed=CHUNKS * 3 * inner * width * 2, transcendentals=total * inner),
        )(seq_lens, tokens.reshape(total, width), w_q, w_k, w_v, w_o, w_gate, w_up, w_down,
          g_q[None], g_k[None], g_attn[None], g_mlp[None], jnp.asarray(cos), jnp.asarray(sin))
        cache = (prompts, 1, seq_len, HEAD_DIM)
        return y.reshape(prompts, seq_len, width), keys.reshape(cache), v.reshape(cache)

    return jax.shard_map(local_layer, mesh=mesh, in_specs=(P('dp', None, None), P('dp'), P(None, 'tp'), P(None, 'tp'), P(None, 'tp'), P('tp', None), P('tp'), P('tp'), P(), P(), P(None, 'tp'), P(None, 'tp'), P('tp', None)), out_specs=(P('dp', None, None), P('dp', 'tp', None, None), P('dp', 'tp', None, None)), check_vma=False)
```

```python
import functools

import jax
import jax.numpy as jnp
import numpy as np
from jax import lax
from jax.experimental import pallas as pl
from jax.experimental.pallas import tpu as pltpu
from jax.sharding import PartitionSpec as P

HEAD_DIM = 128
ROPE_BASE = 500000.0
NORM_EPS = 1e-6
MESH = pl.DeviceIdType.MESH
CHUNKS = 4
GU = 384
DN = 512
BLK = 16
STAT = 128

PROLOGUE, STEPS = 22, 107
EVENTS = {
    (2, 0): (2, 7, 18, 21),
    (2, 1): (2, 12, 20, 23),
    (0, 6): (22, 40, 60, 76),
    (0, 5): (20, 36, 53, 71),
    (0, 4): (15, 29, 43, 65),
    (0, 3): (12, 24, 31, 56),
    (0, 2): (7, 23, 28, 45),
    (0, 1): (4, 18, 25, 31),
    (0, 0): (2, 13, 23, 28),
    (1, 6): (99, 101, 103, 106),
    (1, 5): (98, 99, 101, 105),
    (1, 4): (69, 85, 93, 104),
    (1, 3): (61, 79, 88, 101),
    (1, 2): (53, 73, 84, 100),
    (1, 1): (44, 62, 80, 98),
}


def rope_tables(seq_len, head_dim):
    half_dim = head_dim // 2
    inv_freq = np.float32(ROPE_BASE) ** (np.float32(-2.0) * np.arange(half_dim, dtype=np.float32) / np.float32(head_dim))
    angles = np.arange(seq_len, dtype=np.float32)[:, None] * inv_freq[None, :].astype(np.float32)
    cos, sin = np.cos(angles).astype(np.float32), np.sin(angles).astype(np.float32)
    return np.concatenate([cos, cos], axis=-1), np.concatenate([-sin, sin], axis=-1)


def rms_scale(vals):
    return lax.rsqrt(jnp.mean(vals * vals, axis=-1, keepdims=True) + NORM_EPS)


def post_norm(base, branch, gain):
    branch32 = branch.astype(jnp.float32)
    return (base.astype(jnp.float32) + branch32 * rms_scale(branch32) * gain.astype(jnp.float32)).astype(jnp.bfloat16)


def layer_kernel(seq_len, tp_size, lens_ref, x_ref, wq_ref, wk_ref, wv_ref, wo_ref, wg_ref, wu_ref, wd_ref,
                 gq_ref, gk_ref, ga_ref, gm_ref, cos_ref, sin_ref, y_ref, kc_ref, vc_ref,
                 wgu, wdb, h, act, part, r0, r1, r2, obuf, qk, ho, yo, stat, stat_in, inv,
                 gu_sem, wd_sem, wo_sem, wqkv_sem, x_sem, ho_sem, yo_sem, st_send, st_recv, send, recv, free, hfree):
    size, width = part.shape
    q_width = obuf.shape[1]
    group = q_width // HEAD_DIM
    gu_tiles = wg_ref.shape[1] // GU
    dn_tiles = width // DN
    per_slot = dn_tiles // 2
    per_chunk = gu_tiles + dn_tiles
    me = lax.axis_index('tp')
    core = lax.rem(me, 2)
    xi = lax.rem(lax.div(me, 2), 2)
    yi = lax.div(me, 4)
    partners = (me + 1 - 2 * core, me + 2 - 4 * xi, me + 4 - 8 * yi)
    core_dev = partners[0]
    parts = 4
    quarter = size // parts
    n0, n1, n2 = quarter // 2, quarter // 4, quarter // 8
    first, second = (xi, yi), (yi, xi)
    first_dev, second_dev = partners[1:], partners[:0:-1]

    barrier = pltpu.get_barrier_semaphore()
    for r in range(1, tp_size):
        pl.semaphore_signal(barrier, inc=1, device_id={'tp': lax.rem(me + r, tp_size)}, device_id_type=MESH)

    def rows(start, count):
        return pl.ds(pl.multiple_of(start, BLK), count)

    def remote(stream, phase, p, chunk):
        col = p % 2
        a = p * quarter + core * n0
        b = a + first[col] * n1
        own = b + second[col] * n2
        if phase == 0:
            src, dst, dev = part.at[rows(p * quarter + (1 - core) * n0, n0)], r0.at[stream, pl.ds(p * n0, n0)], core_dev
        elif phase == 1:
            src, dst, dev = r0.at[stream, rows(p * n0 + (1 - first[col]) * n1, n1)], r1.at[stream, pl.ds(p * n1, n1)], first_dev[col]
        elif phase == 2:
            src, dst, dev = r1.at[stream, rows(p * n1 + (1 - second[col]) * n2, n2)], r2.at[stream, pl.ds(p * n2, n2)], second_dev[col]
        else:
            start, count, dev = ((own, n2, second_dev[col]), (b, n1, first_dev[col]), (a, n0, core_dev))[phase - 3]
            if stream == 0:
                src = dst = h.at[lax.rem(chunk, 2), rows(start, count)]
            else:
                dst = y_ref.at[rows(chunk * size + start, count)]
                src = yo.at[pl.ds(p * n2, n2)] if phase == 3 else dst
        return pltpu.make_async_remote_copy(src_ref=src, dst_ref=dst, send_sem=send.at[stream, chunk, phase, p], recv_sem=recv.at[stream, chunk, phase, p], device_id={'tp': dev}, device_id_type=MESH)

    def own_row(p):
        return p * quarter + core * n0 + first[p % 2] * n1 + second[p % 2] * n2

    def base_copy(p, chunk):
        return pltpu.make_async_copy(x_ref.at[rows(chunk * size + own_row(p), n2)], ho.at[chunk, pl.ds(p * n2, n2)], ho_sem.at[chunk, p])

    def y_copy(p, chunk):
        return pltpu.make_async_copy(yo.at[pl.ds(p * n2, n2)], y_ref.at[rows(chunk * size + own_row(p), n2)], yo_sem.at[p])

    def x_copy(chunk):
        return pltpu.make_async_copy(x_ref.at[rows(chunk * size, size)], h.at[1], x_sem)

    def wo_copies():
        return [pltpu.make_async_copy(wo_ref.at[:, pl.ds(k * DN, DN)], wdb.at[k // per_slot, pl.ds(k % per_slot * q_width, q_width)], wo_sem.at[k]) for k in range(dn_tiles)]

    def qkv_copies():
        return (pltpu.make_async_copy(wq_ref, wgu.at[0, :, pl.ds(0, q_width)], wqkv_sem.at[0]),
                pltpu.make_async_copy(wk_ref, wgu.at[0, :, pl.ds(q_width, HEAD_DIM)], wqkv_sem.at[1]),
                pltpu.make_async_copy(wv_ref, wgu.at[1, :, pl.ds(0, HEAD_DIM)], wqkv_sem.at[2]))

    def gu_copies(chunk, j):
        slot = lax.rem(chunk * gu_tiles + j, 2)
        cols = pl.ds(pl.multiple_of(j * GU, GU), GU)
        depth = width // 2
        return [pltpu.make_async_copy(w.at[pl.ds(b * depth, depth), cols], wgu.at[slot, pl.ds(b * depth, depth), pl.ds(a * GU, GU)], gu_sem.at[slot, a, b])
                for a, w in enumerate((wg_ref, wu_ref)) for b in range(2)]

    def dn_copies(k):
        slot, depth = lax.rem(k, 2), wd_ref.shape[0] // 2
        cols = pl.ds(pl.multiple_of(k * DN, DN), DN)
        return [pltpu.make_async_copy(wd_ref.at[pl.ds(b * depth, depth), cols], wdb.at[slot, pl.ds(b * depth, depth)], wd_sem.at[slot, b]) for b in range(2)]

    def launch(copies):
        for cp in copies:
            cp.start()

    def stat_copy(r, chunk):
        return pltpu.make_async_remote_copy(src_ref=stat.at[chunk], dst_ref=stat_in.at[chunk, r - 1], send_sem=st_send.at[chunk, r - 1], recv_sem=st_recv.at[chunk, r - 1], device_id={'tp': lax.rem(me + r, tp_size)}, device_id_type=MESH)

    def release_h():
        for i, dev in enumerate(partners):
            pl.semaphore_signal(hfree.at[i], inc=1, device_id={'tp': dev}, device_id_type=MESH)

    def add_into(dst, dst_start, src, src_start, count):
        @pl.loop(0, count // BLK)
        def _(i):
            d = pl.ds(pl.multiple_of(dst_start + i * BLK, BLK), BLK)
            s = pl.ds(pl.multiple_of(src_start + i * BLK, BLK), BLK)
            dst[d, :] = (dst[d, :].astype(jnp.float32) + src[s, :].astype(jnp.float32)).astype(jnp.bfloat16)

    def project_qkv(chunk):
        @pl.when(chunk == 0)
        def _():
            for cp in qkv_copies():
                cp.wait()
        x_copy(chunk).wait()
        qk[...] = jnp.dot(h[1], wgu[0], preferred_element_type=jnp.float32)
        vc_ref[rows(chunk * size, size), :] = jnp.dot(h[1], wgu[1, :, pl.ds(0, HEAD_DIM)], preferred_element_type=jnp.float32).astype(jnp.bfloat16)

        @pl.when(chunk + 1 < CHUNKS)
        def _():
            x_copy(chunk + 1).start()

        @pl.when(chunk + 1 == CHUNKS)
        def _():
            release_h()
            launch(gu_copies(0, 0))
        sums = []
        for blk in range(size // STAT):
            r = pl.ds(blk * STAT, STAT)
            squares = [jnp.square(qk[r, pl.ds(t * HEAD_DIM, HEAD_DIM)]) for t in range(group + 1)]
            for sq in (sum(squares[1:group], squares[0]), squares[group]):
                sums.append(jnp.sum(sq.T, axis=0, keepdims=True))
        stat[chunk] = jnp.concatenate(sums, axis=0)
        for r in range(1, tp_size):
            stat_copy(r, chunk).start()

    def attend(chunk):
        total = stat[chunk]
        for r in range(1, tp_size):
            stat_copy(r, chunk).wait()
        for r in range(1, tp_size):
            total = total + stat_in[chunk, r - 1]
        inv[0] = lax.rsqrt(total / (q_width * tp_size) + NORM_EPS)
        inv[1] = lax.rsqrt(total / (HEAD_DIM * tp_size) + NORM_EPS)
        cos, sin = cos_ref[...], sin_ref[...]
        gk = gk_ref[...].astype(jnp.float32)[None, :]
        row = lax.broadcasted_iota(jnp.int32, (seq_len, seq_len), 0)
        col = lax.broadcasted_iota(jnp.int32, (seq_len, seq_len), 1)

        def rope(t):
            return t * cos + pltpu.roll(t, HEAD_DIM // 2, 1) * sin

        @pl.loop(0, size // STAT)
        def _(blk):
            iq = jnp.broadcast_to(inv[0, pl.ds(2 * blk, 1), :], (STAT, HEAD_DIM)).T
            ik = jnp.broadcast_to(inv[1, pl.ds(2 * blk + 1, 1), :], (STAT, HEAD_DIM)).T
            for b in range(STAT // seq_len):
                local = pl.ds(pl.multiple_of(blk * STAT + b * seq_len, seq_len), seq_len)
                mine = pl.ds(pl.multiple_of(chunk * size + blk * STAT + b * seq_len, seq_len), seq_len)
                inv_q, inv_k = iq[b * seq_len:(b + 1) * seq_len, :], ik[b * seq_len:(b + 1) * seq_len, :]
                keys = rope(qk[local, pl.ds(q_width, HEAD_DIM)] * inv_k * gk).astype(jnp.bfloat16)
                kc_ref[mine, :] = keys
                qs = []
                for hd in range(group):
                    cols = pl.ds(hd * HEAD_DIM, HEAD_DIM)
                    qs.append(rope(qk[local, cols] * inv_q * gq_ref[cols].astype(jnp.float32)[None, :]).astype(jnp.bfloat16))
                queries = jnp.concatenate(qs, axis=0)
                scores = lax.dot_general(queries, keys, (((1,), (1,)), ((), ())), preferred_element_type=jnp.float32) * HEAD_DIM ** -0.5
                length = lens_ref[chunk * (size // seq_len) + blk * (STAT // seq_len) + b]
                allowed = ((col <= row) & (col < length)).astype(jnp.int32)
                scores = jnp.where(jnp.concatenate([allowed] * group, axis=0) > 0, scores, -1e30)
                e = jnp.exp(scores - jnp.max(scores, axis=-1, keepdims=True))
                probs = (e / jnp.sum(e, axis=-1, keepdims=True)).astype(jnp.bfloat16)
                out = jnp.dot(probs, vc_ref[mine, :], preferred_element_type=jnp.float32).astype(jnp.bfloat16)
                for hd in range(group):
                    obuf[mine, pl.ds(hd * HEAD_DIM, HEAD_DIM)] = out[hd * seq_len:(hd + 1) * seq_len, :]

    def project(chunk):
        @pl.when(chunk == 0)
        def _():
            for cp in wo_copies():
                cp.wait()

        @pl.loop(0, dn_tiles)
        def _(k):
            w = wdb[lax.div(k, per_slot), pl.ds(pl.multiple_of(lax.rem(k, per_slot) * q_width, q_width), q_width), :]
            cols = pl.ds(pl.multiple_of(k * DN, DN), DN)
            part[:, cols] = jnp.dot(obuf[rows(chunk * size, size), :], w, preferred_element_type=jnp.float32).astype(jnp.bfloat16)

    def take(sem, chunk):
        @pl.when(chunk >= 1)
        def _():
            pl.semaphore_wait(sem, 1)

    def give(sem, chunk, dev):
        @pl.when(chunk + 1 < CHUNKS)
        def _():
            pl.semaphore_signal(sem, inc=1, device_id={'tp': dev}, device_id_type=MESH)

    def event(stream, e, chunk):
        for p in range(parts):
            col = p % 2
            if e > 0:
                prev = remote(stream, e - 1, p, chunk)
                prev.wait_recv()
                prev.wait_send()
            if e == 1:
                add_into(r0.at[stream], p * n0, part, p * quarter + core * n0, n0)
            elif e == 2:
                add_into(r1.at[stream], p * n1, r0.at[stream], p * n0 + first[col] * n1, n1)
                give(free.at[stream, 0, p], chunk, core_dev)
            elif e == 3:
                gain = ga_ref if stream == 0 else gm_ref
                mine = pl.ds(p * n2, n2)
                kept = rows(p * n1 + second[col] * n2, n2)
                total = (r2[stream, mine, :].astype(jnp.float32) + r1[stream, kept, :].astype(jnp.float32)).astype(jnp.bfloat16)
                if stream == 0:
                    base_copy(p, chunk).wait()
                out = post_norm(ho[chunk, mine, :], total, gain[...][None, :])
                if stream == 0:
                    if p == 0:
                        for i in range(len(partners)):
                            take(hfree.at[i], chunk)
                    h[lax.rem(chunk, 2), rows(own_row(p), n2), :] = out
                    ho[chunk, mine, :] = out
                else:
                    yo[mine, :] = out
                    y_copy(p, chunk).start()
                give(free.at[stream, 1, p], chunk, first_dev[col])
                give(free.at[stream, 2, p], chunk, second_dev[col])
            elif e == 4 and stream == 1:
                y_copy(p, chunk).wait()
            if e < 3:
                take(free.at[stream, e, p], chunk)
            if e < 6:
                remote(stream, e, p, chunk).start()

    for cp in qkv_copies():
        cp.start()
    x_copy(0).start()
    for cp in wo_copies():
        cp.start()
    for chunk in range(CHUNKS):
        for p in range(parts):
            base_copy(p, chunk).start()
    pl.semaphore_wait(barrier, tp_size - 1)

    reload_wo = sorted({(s - PROLOGUE) // per_chunk for s in EVENTS[0, 0] if s >= PROLOGUE} - {0})

    @pl.loop(0, STEPS)
    def _(g):
        gm = g - PROLOGUE
        c, j = lax.div(gm, per_chunk), lax.rem(gm, per_chunk)
        computes = (gm >= 0) & (gm < CHUNKS * per_chunk)

        for it in reload_wo:
            @pl.when(gm == it * per_chunk + 1)
            def _():
                for cp in wo_copies():
                    cp.wait()

        for (stream, e), at in EVENTS.items():
            hit = functools.reduce(lambda a, b: a | b, [g == s for s in at])

            @pl.when(hit)
            def _():
                chunk = sum([(g >= s).astype(jnp.int32) for s in at[1:]])
                if stream == 2:
                    (project_qkv, attend)[e](chunk)
                else:
                    if (stream, e) == (0, 0):
                        project(chunk)
                    event(stream, e, chunk)

        @pl.when(computes & (j < gu_tiles))
        def _():
            for cp in gu_copies(c, j):
                cp.wait()

            @pl.when((j + 1 < gu_tiles) | (c + 1 < CHUNKS))
            def _():
                wraps = (j + 1 >= gu_tiles).astype(jnp.int32)
                launch(gu_copies(c + wraps, (j + 1) * (1 - wraps)))

            @pl.when(j == gu_tiles - 2)
            def _():
                launch(dn_copies(0))
            slot = lax.rem(c * gu_tiles + j, 2)
            both = jnp.dot(h[lax.rem(c, 2)], wgu[slot], preferred_element_type=jnp.float32)
            gate, up = both[:, :GU], both[:, GU:]
            act[:, pl.ds(pl.multiple_of(j * GU, GU), GU)] = (gate * lax.logistic(gate) * up).astype(jnp.bfloat16)

            @pl.when((j == gu_tiles - 1) & (c + 2 < CHUNKS))
            def _():
                release_h()

        @pl.when(computes & (j >= gu_tiles))
        def _():
            k = j - gu_tiles
            for cp in dn_copies(k):
                cp.wait()

            @pl.when(k + 1 < dn_tiles)
            def _():
                launch(dn_copies(k + 1))
            part[:, pl.ds(pl.multiple_of(k * DN, DN), DN)] = jnp.dot(act[...], wdb[lax.rem(k, 2)], preferred_element_type=jnp.float32).astype(jnp.bfloat16)

            @pl.when(k + 1 == dn_tiles)
            def _():
                event(1, 0, c)
            for it in reload_wo:
                @pl.when(gm == it * per_chunk - 1)
                def _():
                    for cp in wo_copies():
                        cp.start()


def store_kernel(y_ref, k_ref, v_ref, y_out, k_out, v_out, buf, kv, get, put):
    pieces, rows = buf.shape[0], buf.shape[1]
    def piece(i):
        return pl.ds(i * rows, rows)
    loads = [pltpu.make_async_copy(src, kv.at[i], get.at[pieces + i]) for i, src in enumerate((k_ref, v_ref))]
    loads += [pltpu.make_async_copy(y_ref.at[piece(i)], buf.at[i], get.at[i]) for i in range(pieces)]
    stores = [pltpu.make_async_copy(kv.at[i], dst, put.at[pieces + i]) for i, dst in enumerate((k_out, v_out))]
    stores += [pltpu.make_async_copy(buf.at[i], y_out.at[piece(i)], put.at[i]) for i in range(pieces)]
    for cp in loads:
        cp.start()
    for load, store in zip(loads, stores):
        load.wait()
        store.start()
    for cp in stores:
        cp.wait()


def store(y, keys, v):
    pieces = 16
    anyspec = pl.BlockSpec(memory_space=pl.ANY)
    dma = pltpu.SemaphoreType.DMA
    return pl.pallas_call(
        store_kernel,
        out_shape=[jax.ShapeDtypeStruct(t.shape, t.dtype) for t in (y, keys, v)],
        in_specs=[anyspec] * 3,
        out_specs=[anyspec] * 3,
        scratch_shapes=[pltpu.VMEM((pieces, y.shape[0] // pieces, y.shape[1]), y.dtype), pltpu.VMEM((2,) + keys.shape, keys.dtype), dma((pieces + 2,)), dma((pieces + 2,))],
        compiler_params=pltpu.CompilerParams(vmem_limit_bytes=67043328),
    )(y, keys, v)


def solution(mesh):
    tp_size = mesh.shape['tp']

    def local_layer(tokens, seq_lens, w_q, w_k, w_v, w_o, g_q, g_k, g_attn, g_mlp, w_gate, w_up, w_down):
        prompts, seq_len, width = tokens.shape
        total, inner, q_width = prompts * seq_len, w_gate.shape[1], w_q.shape[1]
        size = total // CHUNKS
        cos, sin = rope_tables(seq_len, HEAD_DIM)
        bf, f32 = jnp.bfloat16, jnp.float32
        anyspec = pl.BlockSpec(memory_space=pl.ANY)
        vmem = pl.BlockSpec(memory_space=pltpu.VMEM)
        dma, credit = pltpu.SemaphoreType.DMA, pltpu.SemaphoreType.REGULAR
        kv = jax.ShapeDtypeStruct((total, HEAD_DIM), bf)
        y, keys, v = pl.pallas_call(
            functools.partial(layer_kernel, seq_len, tp_size),
            out_shape=[jax.ShapeDtypeStruct((total, width), bf), kv, kv],
            in_specs=[pl.BlockSpec(memory_space=pltpu.SMEM)] + [anyspec] * 8 + [vmem] * 6,
            out_specs=[anyspec, vmem, vmem],
            scratch_shapes=[
                pltpu.VMEM((2, width, 2 * GU), bf), pltpu.VMEM((2, inner, DN), bf), pltpu.VMEM((2, size, width), bf),
                pltpu.VMEM((size, inner), bf), pltpu.VMEM((size, width), bf),
                pltpu.VMEM((2, size // 2, width), bf), pltpu.VMEM((2, size // 4, width), bf), pltpu.VMEM((2, size // 8, width), bf),
                pltpu.VMEM((total, q_width), bf), pltpu.VMEM((size, q_width + HEAD_DIM), f32),
                pltpu.VMEM((CHUNKS, size // 8, width), bf), pltpu.VMEM((size // 8, width), bf),
                pltpu.VMEM((CHUNKS, 8, STAT), f32), pltpu.VMEM((CHUNKS, tp_size - 1, 8, STAT), f32), pltpu.VMEM((2, 8, STAT), f32),
                dma((2, 2, 2)), dma((2, 2)), dma((width // DN,)), dma((3,)), dma, dma((CHUNKS, 4)), dma((4,)),
                dma((CHUNKS, tp_size - 1)), dma((CHUNKS, tp_size - 1)), dma((2, CHUNKS, 6, 4)), dma((2, CHUNKS, 6, 4)),
                credit((2, 3, 4)), credit((3,)),
            ],
            compiler_params=pltpu.CompilerParams(collective_id=0, has_side_effects=True, vmem_limit_bytes=67043328),
            cost_estimate=pl.CostEstimate(flops=2 * total * width * (3 * inner + 2 * q_width + 2 * HEAD_DIM), bytes_accessed=CHUNKS * 3 * inner * width * 2, transcendentals=total * inner),
        )(seq_lens, tokens.reshape(total, width), w_q, w_k, w_v, w_o, w_gate, w_up, w_down,
          g_q, g_k, g_attn, g_mlp, jnp.asarray(cos), jnp.asarray(sin))
        y, keys, v = store(y, keys, v)
        cache = (prompts, 1, seq_len, HEAD_DIM)
        return y.reshape(prompts, seq_len, width), keys.reshape(cache), v.reshape(cache)

    return jax.shard_map(local_layer, mesh=mesh, in_specs=(P('dp', None, None), P('dp'), P(None, 'tp'), P(None, 'tp'), P(None, 'tp'), P('tp', None), P('tp'), P('tp'), P(), P(), P(None, 'tp'), P(None, 'tp'), P('tp', None)), out_specs=(P('dp', None, None), P('dp', 'tp', None, None), P('dp', 'tp', None, None)), check_vma=False)
```

```python
import functools

import jax
import jax.numpy as jnp
import numpy as np
from jax import lax
from jax.experimental import pallas as pl
from jax.experimental.pallas import tpu as pltpu
from jax.sharding import PartitionSpec as P

HEAD_DIM = 128
ROPE_BASE = 500000.0
NORM_EPS = 1e-6
MESH = pl.DeviceIdType.MESH
CHUNKS = 4
GU = 384
DN = 1024
BLK = 16
STAT = 128

PROLOGUE, STEPS = 22, 87
EVENTS = {
    (2, 0): (0, 3, 10, 19),
    (2, 1): (1, 5, 12, 27),
    (0, 6): (22, 36, 48, 64),
    (0, 5): (18, 33, 46, 57),
    (0, 4): (8, 29, 35, 50),
    (0, 3): (5, 24, 31, 45),
    (0, 2): (4, 23, 28, 41),
    (0, 1): (2, 11, 25, 31),
    (0, 0): (1, 6, 23, 28),
    (1, 6): (81, 84, 85, 86),
    (1, 5): (78, 80, 83, 84),
    (1, 4): (52, 67, 75, 83),
    (1, 3): (49, 64, 73, 81),
    (1, 2): (46, 58, 71, 80),
    (1, 1): (37, 51, 65, 78),
}


def rope_tables(seq_len, head_dim):
    half_dim = head_dim // 2
    inv_freq = np.float32(ROPE_BASE) ** (np.float32(-2.0) * np.arange(half_dim, dtype=np.float32) / np.float32(head_dim))
    angles = np.arange(seq_len, dtype=np.float32)[:, None] * inv_freq[None, :].astype(np.float32)
    cos, sin = np.cos(angles).astype(np.float32), np.sin(angles).astype(np.float32)
    return np.concatenate([cos, cos], axis=-1), np.concatenate([-sin, sin], axis=-1)


def rms_scale(vals):
    return lax.rsqrt(jnp.mean(vals * vals, axis=-1, keepdims=True) + NORM_EPS)


def post_norm(base, branch, gain):
    branch32 = branch.astype(jnp.float32)
    return (base.astype(jnp.float32) + branch32 * rms_scale(branch32) * gain.astype(jnp.float32)).astype(jnp.bfloat16)


def layer_kernel(seq_len, tp_size, lens_ref, x_ref, wq_ref, wk_ref, wv_ref, wo_ref, wg_ref, wu_ref, wd_ref,
                 gq_ref, gk_ref, ga_ref, gm_ref, cos_ref, sin_ref, y_ref, kc_ref, vc_ref,
                 wgu, wdb, h, act, part, r0, r1, r2, obuf, qk, kv, ho, stat, stat_in, inv,
                 gu_sem, wd_sem, wo_sem, wqkv_sem, x_sem, kv_sem, ho_sem, yo_sem, st_send, st_recv, send, recv, free, hfree):
    size, width = part.shape
    half = width // 2
    q_width = obuf.shape[1]
    group = q_width // HEAD_DIM
    gu_tiles = wg_ref.shape[1] // GU
    dn_tiles = width // DN
    per_chunk = gu_tiles + dn_tiles
    me = lax.axis_index('tp')
    core = lax.rem(me, 2)
    xi = lax.rem(lax.div(me, 2), 2)
    yi = lax.div(me, 4)
    partners = (me + 1 - 2 * core, me + 2 - 4 * xi, me + 4 - 8 * yi)
    core_dev = partners[0]
    parts = 4
    quarter = size // parts
    n0, n1, n2 = quarter // 2, quarter // 4, quarter // 8
    first, second = (xi, yi), (yi, xi)
    first_dev, second_dev = partners[1:], partners[:0:-1]

    barrier = pltpu.get_barrier_semaphore()
    for r in range(1, tp_size):
        pl.semaphore_signal(barrier, inc=1, device_id={'tp': lax.rem(me + r, tp_size)}, device_id_type=MESH)

    def rows(start, count):
        return pl.ds(pl.multiple_of(start, BLK), count)

    def remote(stream, phase, p, chunk):
        col = p % 2
        a = p * quarter + core * n0
        b = a + first[col] * n1
        own = b + second[col] * n2
        if phase == 0:
            src, dst, dev = part.at[rows(p * quarter + (1 - core) * n0, n0)], r0.at[stream, pl.ds(p * n0, n0)], core_dev
        elif phase == 1:
            src, dst, dev = r0.at[stream, rows(p * n0 + (1 - first[col]) * n1, n1)], r1.at[stream, pl.ds(p * n1, n1)], first_dev[col]
        elif phase == 2:
            src, dst, dev = r1.at[stream, rows(p * n1 + (1 - second[col]) * n2, n2)], r2.at[stream, pl.ds(p * n2, n2)], second_dev[col]
        else:
            start, count, dev = ((own, n2, second_dev[col]), (b, n1, first_dev[col]), (a, n0, core_dev))[phase - 3]
            if stream == 0:
                src = dst = h.at[lax.rem(chunk, 2), :, rows(start, count)]
            else:
                dst = y_ref.at[rows(chunk * size + start, count)]
                src = ho.at[chunk, pl.ds(p * n2, n2)] if phase == 3 else dst
        return pltpu.make_async_remote_copy(src_ref=src, dst_ref=dst, send_sem=send.at[stream, chunk, phase, p], recv_sem=recv.at[stream, chunk, phase, p], device_id={'tp': dev}, device_id_type=MESH)

    def own_row(p):
        return p * quarter + core * n0 + first[p % 2] * n1 + second[p % 2] * n2

    def base_copy(p, chunk):
        return pltpu.make_async_copy(x_ref.at[rows(chunk * size + own_row(p), n2)], ho.at[chunk, pl.ds(p * n2, n2)], ho_sem.at[chunk, p])

    def y_copy(p, chunk):
        return pltpu.make_async_copy(ho.at[chunk, pl.ds(p * n2, n2)], y_ref.at[rows(chunk * size + own_row(p), n2)], yo_sem.at[p])

    def x_copy(chunk):
        return [pltpu.make_async_copy(x_ref.at[rows(chunk * size, size), pl.ds(i * half, half)], h.at[1, i], x_sem.at[i]) for i in range(2)]

    def times_h(par, w):
        return sum(jnp.dot(h[par, i], w[i], preferred_element_type=jnp.float32) for i in range(2))

    def wo_copies():
        return [pltpu.make_async_copy(wo_ref.at[:, dn_cols(k, b)], wdb.at[1, b, pl.ds(k * q_width, q_width)], wo_sem.at[k, b]) for k in range(dn_tiles) for b in range(2)]

    def qkv_copies():
        return (pltpu.make_async_copy(wq_ref, wgu.at[0, :, pl.ds(0, q_width)], wqkv_sem.at[0]),
                pltpu.make_async_copy(wk_ref, wgu.at[0, :, pl.ds(q_width, HEAD_DIM)], wqkv_sem.at[1]),
                pltpu.make_async_copy(wv_ref, wgu.at[1, :, pl.ds(0, HEAD_DIM)], wqkv_sem.at[2]))

    def gu_copies(chunk, j):
        slot = lax.rem(chunk * gu_tiles + j, 2)
        cols = pl.ds(pl.multiple_of(j * GU, GU), GU)
        depth = width // 2
        return [pltpu.make_async_copy(w.at[pl.ds(b * depth, depth), cols], wgu.at[slot, pl.ds(b * depth, depth), pl.ds(a * GU, GU)], gu_sem.at[slot, a, b])
                for a, w in enumerate((wg_ref, wu_ref)) for b in range(2)]

    def dn_cols(k, b):
        return pl.ds(pl.multiple_of(k * DN + b * (DN // 2), DN // 2), DN // 2)

    def dn_copies(k):
        slot = lax.rem(k, 2)
        return [pltpu.make_async_copy(wd_ref.at[:, dn_cols(k, b)], wdb.at[slot, b], wd_sem.at[slot, b]) for b in range(2)]

    def kv_copies(chunk):
        return [pltpu.make_async_copy(kv.at[i], out.at[rows(chunk * size, size)], kv_sem.at[i]) for i, out in enumerate((kc_ref, vc_ref))]

    def launch(copies):
        for cp in copies:
            cp.start()

    def stat_copy(r, chunk):
        return pltpu.make_async_remote_copy(src_ref=stat.at[chunk], dst_ref=stat_in.at[chunk, r - 1], send_sem=st_send.at[chunk, r - 1], recv_sem=st_recv.at[chunk, r - 1], device_id={'tp': lax.rem(me + r, tp_size)}, device_id_type=MESH)

    def release_h():
        for i, dev in enumerate(partners):
            pl.semaphore_signal(hfree.at[i], inc=1, device_id={'tp': dev}, device_id_type=MESH)

    def add_into(dst, dst_start, src, src_start, count):
        @pl.loop(0, count // BLK)
        def _(i):
            d = pl.ds(pl.multiple_of(dst_start + i * BLK, BLK), BLK)
            s = pl.ds(pl.multiple_of(src_start + i * BLK, BLK), BLK)
            dst[d, :] = (dst[d, :].astype(jnp.float32) + src[s, :].astype(jnp.float32)).astype(jnp.bfloat16)

    def project_qkv(chunk):
        @pl.when(chunk == 0)
        def _():
            for cp in qkv_copies():
                cp.wait()
        for cp in x_copy(chunk):
            cp.wait()
        qk[...] = times_h(1, [wgu[0, pl.ds(i * half, half)] for i in range(2)])
        @pl.when(chunk > 0)
        def _():
            for cp in kv_copies(chunk - 1):
                cp.wait()
        kv[1] = times_h(1, [wgu[1, pl.ds(i * half, half), pl.ds(0, HEAD_DIM)] for i in range(2)]).astype(jnp.bfloat16)

        @pl.when(chunk + 1 < CHUNKS)
        def _():
            for cp in x_copy(chunk + 1):
                cp.start()

        @pl.when(chunk + 1 == CHUNKS)
        def _():
            release_h()
            launch(gu_copies(0, 0))
        sums = []
        for blk in range(size // STAT):
            r = pl.ds(blk * STAT, STAT)
            squares = [jnp.square(qk[r, pl.ds(t * HEAD_DIM, HEAD_DIM)]) for t in range(group + 1)]
            for sq in (sum(squares[1:group], squares[0]), squares[group]):
                sums.append(jnp.sum(sq.T, axis=0, keepdims=True))
        stat[chunk] = jnp.concatenate(sums, axis=0)
        for r in range(1, tp_size):
            stat_copy(r, chunk).start()

    def attend(chunk):
        total = stat[chunk]
        for r in range(1, tp_size):
            stat_copy(r, chunk).wait()
        for r in range(1, tp_size):
            total = total + stat_in[chunk, r - 1]
        inv[0] = lax.rsqrt(total / (q_width * tp_size) + NORM_EPS)
        inv[1] = lax.rsqrt(total / (HEAD_DIM * tp_size) + NORM_EPS)
        cos, sin = cos_ref[...], sin_ref[...]
        gk = gk_ref[...].astype(jnp.float32)[None, :]
        row = lax.broadcasted_iota(jnp.int32, (seq_len, seq_len), 0)
        col = lax.broadcasted_iota(jnp.int32, (seq_len, seq_len), 1)

        def rope(t):
            return t * cos + pltpu.roll(t, HEAD_DIM // 2, 1) * sin

        @pl.loop(0, size // STAT)
        def _(blk):
            iq = jnp.broadcast_to(inv[0, pl.ds(2 * blk, 1), :], (STAT, HEAD_DIM)).T
            ik = jnp.broadcast_to(inv[1, pl.ds(2 * blk + 1, 1), :], (STAT, HEAD_DIM)).T
            for b in range(STAT // seq_len):
                local = pl.ds(pl.multiple_of(blk * STAT + b * seq_len, seq_len), seq_len)
                inv_q, inv_k = iq[b * seq_len:(b + 1) * seq_len, :], ik[b * seq_len:(b + 1) * seq_len, :]
                keys = rope(qk[local, pl.ds(q_width, HEAD_DIM)] * inv_k * gk).astype(jnp.bfloat16)
                kv[0, local, :] = keys
                qs = []
                for hd in range(group):
                    cols = pl.ds(hd * HEAD_DIM, HEAD_DIM)
                    qs.append(rope(qk[local, cols] * inv_q * gq_ref[cols].astype(jnp.float32)[None, :]).astype(jnp.bfloat16))
                queries = jnp.concatenate(qs, axis=0)
                scores = lax.dot_general(queries, keys, (((1,), (1,)), ((), ())), preferred_element_type=jnp.float32) * HEAD_DIM ** -0.5
                length = lens_ref[chunk * (size // seq_len) + blk * (STAT // seq_len) + b]
                allowed = ((col <= row) & (col < length)).astype(jnp.int32)
                scores = jnp.where(jnp.concatenate([allowed] * group, axis=0) > 0, scores, -1e30)
                e = jnp.exp(scores - jnp.max(scores, axis=-1, keepdims=True))
                probs = (e / jnp.sum(e, axis=-1, keepdims=True)).astype(jnp.bfloat16)
                out = jnp.dot(probs, kv[1, local, :], preferred_element_type=jnp.float32).astype(jnp.bfloat16)
                for hd in range(group):
                    obuf[local, pl.ds(hd * HEAD_DIM, HEAD_DIM)] = out[hd * seq_len:(hd + 1) * seq_len, :]
        launch(kv_copies(chunk))

    def project(chunk):
        @pl.when(chunk == 0)
        def _():
            for cp in wo_copies():
                cp.wait()

        @pl.loop(0, dn_tiles)
        def _(k):
            for b in range(2):
                w = wdb[1, b, pl.ds(pl.multiple_of(k * q_width, q_width), q_width), :]
                part[:, dn_cols(k, b)] = jnp.dot(obuf[...], w, preferred_element_type=jnp.float32).astype(jnp.bfloat16)

    def take(sem, chunk):
        @pl.when(chunk >= 1)
        def _():
            pl.semaphore_wait(sem, 1)

    def give(sem, chunk, dev):
        @pl.when(chunk + 1 < CHUNKS)
        def _():
            pl.semaphore_signal(sem, inc=1, device_id={'tp': dev}, device_id_type=MESH)

    def event(stream, e, chunk):
        for p in range(parts):
            col = p % 2
            if e > 0:
                prev = remote(stream, e - 1, p, chunk)
                prev.wait_recv()
                prev.wait_send()
            if e == 1:
                add_into(r0.at[stream], p * n0, part, p * quarter + core * n0, n0)
            elif e == 2:
                add_into(r1.at[stream], p * n1, r0.at[stream], p * n0 + first[col] * n1, n1)
                give(free.at[stream, 0, p], chunk, core_dev)
            elif e == 3:
                gain = ga_ref if stream == 0 else gm_ref
                mine = pl.ds(p * n2, n2)
                kept = rows(p * n1 + second[col] * n2, n2)
                total = (r2[stream, mine, :].astype(jnp.float32) + r1[stream, kept, :].astype(jnp.float32)).astype(jnp.bfloat16)
                if stream == 0:
                    base_copy(p, chunk).wait()
                out = post_norm(ho[chunk, mine, :], total, gain[...][None, :])
                if stream == 0:
                    if p == 0:
                        for i in range(len(partners)):
                            take(hfree.at[i], chunk)
                    for i in range(2):
                        h[lax.rem(chunk, 2), i, rows(own_row(p), n2), :] = out[:, i * half:(i + 1) * half]
                ho[chunk, mine, :] = out
                if stream == 1:
                    y_copy(p, chunk).start()
                give(free.at[stream, 1, p], chunk, first_dev[col])
                give(free.at[stream, 2, p], chunk, second_dev[col])
            elif e == 4 and stream == 1:
                y_copy(p, chunk).wait()
            if e < 3:
                take(free.at[stream, e, p], chunk)
            if e < 6:
                remote(stream, e, p, chunk).start()

    for cp in qkv_copies():
        cp.start()
    for cp in x_copy(0):
        cp.start()
    for cp in wo_copies():
        cp.start()
    for chunk in range(CHUNKS):
        for p in range(parts):
            base_copy(p, chunk).start()
    pl.semaphore_wait(barrier, tp_size - 1)

    reload_wo = sorted({(s - PROLOGUE) // per_chunk for s in EVENTS[0, 0] if s >= PROLOGUE} - {0})

    @pl.loop(0, STEPS)
    def _(g):
        gm = g - PROLOGUE
        c, j = lax.div(gm, per_chunk), lax.rem(gm, per_chunk)
        computes = (gm >= 0) & (gm < CHUNKS * per_chunk)

        for it in reload_wo:
            @pl.when(gm == it * per_chunk + 1)
            def _():
                for cp in wo_copies():
                    cp.wait()

        for (stream, e), at in EVENTS.items():
            hit = functools.reduce(lambda a, b: a | b, [g == s for s in at])

            @pl.when(hit)
            def _():
                chunk = sum([(g >= s).astype(jnp.int32) for s in at[1:]])
                if stream == 2:
                    (project_qkv, attend)[e](chunk)
                else:
                    if (stream, e) == (0, 0):
                        project(chunk)
                    event(stream, e, chunk)

        @pl.when(computes & (j < gu_tiles))
        def _():
            for cp in gu_copies(c, j):
                cp.wait()

            @pl.when((j + 1 < gu_tiles) | (c + 1 < CHUNKS))
            def _():
                wraps = (j + 1 >= gu_tiles).astype(jnp.int32)
                launch(gu_copies(c + wraps, (j + 1) * (1 - wraps)))

            @pl.when(j == gu_tiles - 2)
            def _():
                launch(dn_copies(0))
            slot = lax.rem(c * gu_tiles + j, 2)
            both = times_h(lax.rem(c, 2), [wgu[slot, pl.ds(i * half, half)] for i in range(2)])
            gate, up = both[:, :GU], both[:, GU:]
            act[:, pl.ds(pl.multiple_of(j * GU, GU), GU)] = (gate * lax.logistic(gate) * up).astype(jnp.bfloat16)

            @pl.when((j == gu_tiles - 1) & (c + 2 < CHUNKS))
            def _():
                release_h()

        @pl.when(computes & (j >= gu_tiles))
        def _():
            k = j - gu_tiles
            for cp in dn_copies(k):
                cp.wait()

            @pl.when(k + 1 < dn_tiles)
            def _():
                launch(dn_copies(k + 1))
            for b in range(2):
                part[:, dn_cols(k, b)] = jnp.dot(act[...], wdb[lax.rem(k, 2), b], preferred_element_type=jnp.float32).astype(jnp.bfloat16)

            @pl.when(k + 1 == dn_tiles)
            def _():
                event(1, 0, c)
            for it in reload_wo:
                @pl.when(gm == it * per_chunk - 1)
                def _():
                    for cp in wo_copies():
                        cp.start()

    for cp in kv_copies(CHUNKS - 1):
        cp.wait()


def store_kernel(y_ref, k_ref, v_ref, y_out, k_out, v_out, buf, kv, get, put):
    pieces, rows = buf.shape[0], buf.shape[1]
    def piece(i):
        return pl.ds(i * rows, rows)
    loads = [pltpu.make_async_copy(src, kv.at[i], get.at[pieces + i]) for i, src in enumerate((k_ref, v_ref))]
    loads += [pltpu.make_async_copy(y_ref.at[piece(i)], buf.at[i], get.at[i]) for i in range(pieces)]
    stores = [pltpu.make_async_copy(kv.at[i], dst, put.at[pieces + i]) for i, dst in enumerate((k_out, v_out))]
    stores += [pltpu.make_async_copy(buf.at[i], y_out.at[piece(i)], put.at[i]) for i in range(pieces)]
    for cp in loads:
        cp.start()
    for load, store in zip(loads, stores):
        load.wait()
        store.start()
    for cp in stores:
        cp.wait()


def store(y, keys, v):
    pieces = 16
    anyspec = pl.BlockSpec(memory_space=pl.ANY)
    dma = pltpu.SemaphoreType.DMA
    return pl.pallas_call(
        store_kernel,
        out_shape=[jax.ShapeDtypeStruct(t.shape, t.dtype) for t in (y, keys, v)],
        in_specs=[anyspec] * 3,
        out_specs=[anyspec] * 3,
        scratch_shapes=[pltpu.VMEM((pieces, y.shape[0] // pieces, y.shape[1]), y.dtype), pltpu.VMEM((2,) + keys.shape, keys.dtype), dma((pieces + 2,)), dma((pieces + 2,))],
        compiler_params=pltpu.CompilerParams(vmem_limit_bytes=67043328),
    )(y, keys, v)


def solution(mesh):
    tp_size = mesh.shape['tp']

    def local_layer(tokens, seq_lens, w_q, w_k, w_v, w_o, g_q, g_k, g_attn, g_mlp, w_gate, w_up, w_down):
        prompts, seq_len, width = tokens.shape
        total, inner, q_width = prompts * seq_len, w_gate.shape[1], w_q.shape[1]
        size = total // CHUNKS
        cos, sin = rope_tables(seq_len, HEAD_DIM)
        bf, f32 = jnp.bfloat16, jnp.float32
        anyspec = pl.BlockSpec(memory_space=pl.ANY)
        vmem = pl.BlockSpec(memory_space=pltpu.VMEM)
        dma, credit = pltpu.SemaphoreType.DMA, pltpu.SemaphoreType.REGULAR
        cache_shape = jax.ShapeDtypeStruct((total, HEAD_DIM), bf)
        y, keys, v = pl.pallas_call(
            functools.partial(layer_kernel, seq_len, tp_size),
            out_shape=[jax.ShapeDtypeStruct((total, width), bf), cache_shape, cache_shape],
            in_specs=[pl.BlockSpec(memory_space=pltpu.SMEM)] + [anyspec] * 8 + [vmem] * 6,
            out_specs=[anyspec] * 3,
            scratch_shapes=[
                pltpu.VMEM((2, width, 2 * GU), bf), pltpu.VMEM((2, 2, inner, DN // 2), bf), pltpu.VMEM((2, 2, size, width // 2), bf),
                pltpu.VMEM((size, inner), bf), pltpu.VMEM((size, width), bf),
                pltpu.VMEM((2, size // 2, width), bf), pltpu.VMEM((2, size // 4, width), bf), pltpu.VMEM((2, size // 8, width), bf),
                pltpu.VMEM((size, q_width), bf), pltpu.VMEM((size, q_width + HEAD_DIM), f32), pltpu.VMEM((2, size, HEAD_DIM), bf),
                pltpu.VMEM((CHUNKS, size // 8, width), bf),
                pltpu.VMEM((CHUNKS, 8, STAT), f32), pltpu.VMEM((CHUNKS, tp_size - 1, 8, STAT), f32), pltpu.VMEM((2, 8, STAT), f32),
                dma((2, 2, 2)), dma((2, 2)), dma((width // DN, 2)), dma((3,)), dma((2,)), dma((2,)), dma((CHUNKS, 4)), dma((4,)),
                dma((CHUNKS, tp_size - 1)), dma((CHUNKS, tp_size - 1)), dma((2, CHUNKS, 6, 4)), dma((2, CHUNKS, 6, 4)),
                credit((2, 3, 4)), credit((3,)),
            ],
            compiler_params=pltpu.CompilerParams(collective_id=0, has_side_effects=True, vmem_limit_bytes=67043328),
            cost_estimate=pl.CostEstimate(flops=2 * total * width * (3 * inner + 2 * q_width + 2 * HEAD_DIM), bytes_accessed=CHUNKS * 3 * inner * width * 2, transcendentals=total * inner),
        )(seq_lens, tokens.reshape(total, width), w_q, w_k, w_v, w_o, w_gate, w_up, w_down,
          g_q, g_k, g_attn, g_mlp, jnp.asarray(cos), jnp.asarray(sin))
        y, keys, v = store(y, keys, v)
        cache = (prompts, 1, seq_len, HEAD_DIM)
        return y.reshape(prompts, seq_len, width), keys.reshape(cache), v.reshape(cache)

    return jax.shard_map(local_layer, mesh=mesh, in_specs=(P('dp', None, None), P('dp'), P(None, 'tp'), P(None, 'tp'), P(None, 'tp'), P('tp', None), P('tp'), P('tp'), P(), P(), P(None, 'tp'), P(None, 'tp'), P('tp', None)), out_specs=(P('dp', None, None), P('dp', 'tp', None, None), P('dp', 'tp', None, None)), check_vma=False)
```

```python
import functools

import jax
import jax.numpy as jnp
import numpy as np
from jax import lax
from jax.experimental import pallas as pl
from jax.experimental.pallas import tpu as pltpu
from jax.sharding import PartitionSpec as P

HEAD_DIM = 128
ROPE_BASE = 500000.0
NORM_EPS = 1e-6
MESH = pl.DeviceIdType.MESH
CHUNKS = 4
GU = 384
DN = 1024
BLK = 16
STAT = 128

PROLOGUE, STEPS = 22, 87
EVENTS = {
    (2, 0): (0, 3, 10, 19),
    (2, 1): (1, 5, 12, 27),
    (0, 6): (22, 36, 48, 64),
    (0, 5): (18, 33, 46, 57),
    (0, 4): (8, 29, 35, 50),
    (0, 3): (5, 24, 31, 45),
    (0, 2): (4, 23, 28, 41),
    (0, 1): (2, 11, 25, 31),
    (0, 0): (1, 6, 23, 28),
    (1, 6): (81, 84, 85, 86),
    (1, 5): (78, 80, 83, 84),
    (1, 4): (52, 67, 75, 83),
    (1, 3): (49, 64, 73, 81),
    (1, 2): (46, 58, 71, 80),
    (1, 1): (37, 51, 65, 78),
}


def rope_tables(seq_len, head_dim):
    half_dim = head_dim // 2
    inv_freq = np.float32(ROPE_BASE) ** (np.float32(-2.0) * np.arange(half_dim, dtype=np.float32) / np.float32(head_dim))
    angles = np.arange(seq_len, dtype=np.float32)[:, None] * inv_freq[None, :].astype(np.float32)
    cos, sin = np.cos(angles).astype(np.float32), np.sin(angles).astype(np.float32)
    return np.concatenate([cos, cos], axis=-1), np.concatenate([-sin, sin], axis=-1)


def rms_scale(vals):
    return lax.rsqrt(jnp.mean(vals * vals, axis=-1, keepdims=True) + NORM_EPS)


def post_norm(base, branch, gain):
    branch32 = branch.astype(jnp.float32)
    return (base.astype(jnp.float32) + branch32 * rms_scale(branch32) * gain.astype(jnp.float32)).astype(jnp.bfloat16)


def layer_kernel(seq_len, tp_size, lens_ref, x_ref, wq_ref, wk_ref, wv_ref, wo_ref, wg_ref, wu_ref, wd_ref,
                 gq_ref, gk_ref, ga_ref, gm_ref, cos_ref, sin_ref, y_ref, kc_ref, vc_ref,
                 wgu, wdb, h, act, part, r0, r1, r2, obuf, qk, kv, ho, stat, stat_in, inv,
                 gu_sem, wd_sem, wo_sem, wqkv_sem, x_sem, kv_sem, ho_sem, yo_sem, st_send, st_recv, send, recv, free, hfree):
    size, width = part.shape
    half = width // 2
    q_width = obuf.shape[1]
    group = q_width // HEAD_DIM
    gu_tiles = wg_ref.shape[1] // GU
    dn_tiles = width // DN
    per_chunk = gu_tiles + dn_tiles
    me = lax.axis_index('tp')
    core = lax.rem(me, 2)
    xi = lax.rem(lax.div(me, 2), 2)
    yi = lax.div(me, 4)
    partners = (me + 1 - 2 * core, me + 2 - 4 * xi, me + 4 - 8 * yi)
    core_dev = partners[0]
    parts = 4
    quarter = size // parts
    n0, n1, n2 = quarter // 2, quarter // 4, quarter // 8
    first, second = (xi, yi), (yi, xi)
    first_dev, second_dev = partners[1:], partners[:0:-1]

    barrier = pltpu.get_barrier_semaphore()
    for r in range(1, tp_size):
        pl.semaphore_signal(barrier, inc=1, device_id={'tp': lax.rem(me + r, tp_size)}, device_id_type=MESH)

    def rows(start, count):
        return pl.ds(pl.multiple_of(start, BLK), count)

    def remote(stream, phase, p, chunk):
        col = p % 2
        a = p * quarter + core * n0
        b = a + first[col] * n1
        own = b + second[col] * n2
        if phase == 0:
            src, dst, dev = part.at[rows(p * quarter + (1 - core) * n0, n0)], r0.at[stream, pl.ds(p * n0, n0)], core_dev
        elif phase == 1:
            src, dst, dev = r0.at[stream, rows(p * n0 + (1 - first[col]) * n1, n1)], r1.at[stream, pl.ds(p * n1, n1)], first_dev[col]
        elif phase == 2:
            src, dst, dev = r1.at[stream, rows(p * n1 + (1 - second[col]) * n2, n2)], r2.at[stream, pl.ds(p * n2, n2)], second_dev[col]
        else:
            start, count, dev = ((own, n2, second_dev[col]), (b, n1, first_dev[col]), (a, n0, core_dev))[phase - 3]
            if stream == 0:
                src = dst = h.at[lax.rem(chunk, 2), :, rows(start, count)]
            else:
                dst = y_ref.at[rows(chunk * size + start, count)]
                src = ho.at[chunk, pl.ds(p * n2, n2)] if phase == 3 else dst
        return pltpu.make_async_remote_copy(src_ref=src, dst_ref=dst, send_sem=send.at[stream, chunk, phase, p], recv_sem=recv.at[stream, chunk, phase, p], device_id={'tp': dev}, device_id_type=MESH)

    def own_row(p):
        return p * quarter + core * n0 + first[p % 2] * n1 + second[p % 2] * n2

    def base_copy(p, chunk):
        return pltpu.make_async_copy(x_ref.at[rows(chunk * size + own_row(p), n2)], ho.at[chunk, pl.ds(p * n2, n2)], ho_sem.at[chunk, p])

    def y_copy(p, chunk):
        return pltpu.make_async_copy(ho.at[chunk, pl.ds(p * n2, n2)], y_ref.at[rows(chunk * size + own_row(p), n2)], yo_sem.at[p])

    def x_copy(chunk):
        return [pltpu.make_async_copy(x_ref.at[rows(chunk * size, size), pl.ds(i * half, half)], h.at[1, i], x_sem.at[i]) for i in range(2)]

    def times_h(par, w):
        return sum(jnp.dot(h[par, i], w[i], preferred_element_type=jnp.float32) for i in range(2))

    def wo_copies():
        return [pltpu.make_async_copy(wo_ref.at[:, dn_cols(k, b)], wdb.at[1, b, pl.ds(k * q_width, q_width)], wo_sem.at[k, b]) for k in range(dn_tiles) for b in range(2)]

    def qkv_copies():
        return (pltpu.make_async_copy(wq_ref, wgu.at[0, :, pl.ds(0, q_width)], wqkv_sem.at[0]),
                pltpu.make_async_copy(wk_ref, wgu.at[0, :, pl.ds(q_width, HEAD_DIM)], wqkv_sem.at[1]),
                pltpu.make_async_copy(wv_ref, wgu.at[1, :, pl.ds(0, HEAD_DIM)], wqkv_sem.at[2]))

    def gu_copies(chunk, j):
        slot = lax.rem(chunk * gu_tiles + j, 2)
        cols = pl.ds(pl.multiple_of(j * GU, GU), GU)
        depth = width // 2
        return [pltpu.make_async_copy(w.at[pl.ds(b * depth, depth), cols], wgu.at[slot, pl.ds(b * depth, depth), pl.ds(a * GU, GU)], gu_sem.at[slot, a, b])
                for a, w in enumerate((wg_ref, wu_ref)) for b in range(2)]

    def dn_cols(k, b):
        return pl.ds(pl.multiple_of(k * DN + b * (DN // 2), DN // 2), DN // 2)

    def dn_copies(k):
        slot = lax.rem(k, 2)
        return [pltpu.make_async_copy(wd_ref.at[:, dn_cols(k, b)], wdb.at[slot, b], wd_sem.at[slot, b]) for b in range(2)]

    def kv_copies(chunk):
        return [pltpu.make_async_copy(kv.at[i], out.at[rows(chunk * size, size)], kv_sem.at[i]) for i, out in enumerate((kc_ref, vc_ref))]

    def launch(copies):
        for cp in copies:
            cp.start()

    def stat_copy(r, chunk):
        return pltpu.make_async_remote_copy(src_ref=stat.at[chunk], dst_ref=stat_in.at[chunk, r - 1], send_sem=st_send.at[chunk, r - 1], recv_sem=st_recv.at[chunk, r - 1], device_id={'tp': lax.rem(me + r, tp_size)}, device_id_type=MESH)

    def release_h():
        for i, dev in enumerate(partners):
            pl.semaphore_signal(hfree.at[i], inc=1, device_id={'tp': dev}, device_id_type=MESH)

    def add_into(dst, dst_start, src, src_start, count):
        @pl.loop(0, count // BLK)
        def _(i):
            d = pl.ds(pl.multiple_of(dst_start + i * BLK, BLK), BLK)
            s = pl.ds(pl.multiple_of(src_start + i * BLK, BLK), BLK)
            dst[d, :] = dst[d, :] + src[s, :]

    def project_qkv(chunk):
        @pl.when(chunk == 0)
        def _():
            for cp in qkv_copies():
                cp.wait()
        for cp in x_copy(chunk):
            cp.wait()
        qk[...] = times_h(1, [wgu[0, pl.ds(i * half, half)] for i in range(2)])
        @pl.when(chunk > 0)
        def _():
            for cp in kv_copies(chunk - 1):
                cp.wait()
        kv[1] = times_h(1, [wgu[1, pl.ds(i * half, half), pl.ds(0, HEAD_DIM)] for i in range(2)]).astype(jnp.bfloat16)

        @pl.when(chunk + 1 < CHUNKS)
        def _():
            for cp in x_copy(chunk + 1):
                cp.start()

        @pl.when(chunk + 1 == CHUNKS)
        def _():
            release_h()
            launch(gu_copies(0, 0))
        sums = []
        for blk in range(size // STAT):
            r = pl.ds(blk * STAT, STAT)
            squares = [jnp.square(qk[r, pl.ds(t * HEAD_DIM, HEAD_DIM)]) for t in range(group + 1)]
            for sq in (sum(squares[1:group], squares[0]), squares[group]):
                sums.append(jnp.sum(sq.T, axis=0, keepdims=True))
        stat[chunk] = jnp.concatenate(sums, axis=0)
        for r in range(1, tp_size):
            stat_copy(r, chunk).start()

    def attend(chunk):
        total = stat[chunk]
        for r in range(1, tp_size):
            stat_copy(r, chunk).wait()
        for r in range(1, tp_size):
            total = total + stat_in[chunk, r - 1]
        inv[0] = lax.rsqrt(total / (q_width * tp_size) + NORM_EPS)
        inv[1] = lax.rsqrt(total / (HEAD_DIM * tp_size) + NORM_EPS)
        cos, sin = cos_ref[...], sin_ref[...]
        gk = gk_ref[...].astype(jnp.float32)[None, :]
        row = lax.broadcasted_iota(jnp.int32, (seq_len, seq_len), 0)
        col = lax.broadcasted_iota(jnp.int32, (seq_len, seq_len), 1)

        def rope(t):
            return t * cos + pltpu.roll(t, HEAD_DIM // 2, 1) * sin

        @pl.loop(0, size // STAT)
        def _(blk):
            iq = jnp.broadcast_to(inv[0, pl.ds(2 * blk, 1), :], (STAT, HEAD_DIM)).T
            ik = jnp.broadcast_to(inv[1, pl.ds(2 * blk + 1, 1), :], (STAT, HEAD_DIM)).T
            for b in range(STAT // seq_len):
                local = pl.ds(pl.multiple_of(blk * STAT + b * seq_len, seq_len), seq_len)
                inv_q, inv_k = iq[b * seq_len:(b + 1) * seq_len, :], ik[b * seq_len:(b + 1) * seq_len, :]
                keys = rope(qk[local, pl.ds(q_width, HEAD_DIM)] * inv_k * gk).astype(jnp.bfloat16)
                kv[0, local, :] = keys
                qs = []
                for hd in range(group):
                    cols = pl.ds(hd * HEAD_DIM, HEAD_DIM)
                    qs.append(rope(qk[local, cols] * inv_q * gq_ref[cols].astype(jnp.float32)[None, :]).astype(jnp.bfloat16))
                queries = jnp.concatenate(qs, axis=0)
                scores = lax.dot_general(queries, keys, (((1,), (1,)), ((), ())), preferred_element_type=jnp.float32) * HEAD_DIM ** -0.5
                length = lens_ref[chunk * (size // seq_len) + blk * (STAT // seq_len) + b]
                allowed = ((col <= row) & (col < length)).astype(jnp.int32)
                scores = jnp.where(jnp.concatenate([allowed] * group, axis=0) > 0, scores, -1e30)
                e = jnp.exp(scores - jnp.max(scores, axis=-1, keepdims=True))
                probs = (e / jnp.sum(e, axis=-1, keepdims=True)).astype(jnp.bfloat16)
                out = jnp.dot(probs, kv[1, local, :], preferred_element_type=jnp.float32).astype(jnp.bfloat16)
                for hd in range(group):
                    obuf[local, pl.ds(hd * HEAD_DIM, HEAD_DIM)] = out[hd * seq_len:(hd + 1) * seq_len, :]
        launch(kv_copies(chunk))

    def project(chunk):
        @pl.when(chunk == 0)
        def _():
            for cp in wo_copies():
                cp.wait()

        @pl.loop(0, dn_tiles)
        def _(k):
            for b in range(2):
                w = wdb[1, b, pl.ds(pl.multiple_of(k * q_width, q_width), q_width), :]
                part[:, dn_cols(k, b)] = jnp.dot(obuf[...], w, preferred_element_type=jnp.float32).astype(jnp.bfloat16)

    def take(sem, chunk):
        @pl.when(chunk >= 1)
        def _():
            pl.semaphore_wait(sem, 1)

    def give(sem, chunk, dev):
        @pl.when(chunk + 1 < CHUNKS)
        def _():
            pl.semaphore_signal(sem, inc=1, device_id={'tp': dev}, device_id_type=MESH)

    def event(stream, e, chunk):
        for p in range(parts):
            col = p % 2
            if e > 0:
                prev = remote(stream, e - 1, p, chunk)
                prev.wait_recv()
                prev.wait_send()
            if e == 1:
                add_into(r0.at[stream], p * n0, part, p * quarter + core * n0, n0)
            elif e == 2:
                add_into(r1.at[stream], p * n1, r0.at[stream], p * n0 + first[col] * n1, n1)
                give(free.at[stream, 0, p], chunk, core_dev)
            elif e == 3:
                gain = ga_ref if stream == 0 else gm_ref
                mine = pl.ds(p * n2, n2)
                kept = rows(p * n1 + second[col] * n2, n2)
                total = (r2[stream, mine, :].astype(jnp.float32) + r1[stream, kept, :].astype(jnp.float32)).astype(jnp.bfloat16)
                if stream == 0:
                    base_copy(p, chunk).wait()
                out = post_norm(ho[chunk, mine, :], total, gain[...][None, :])
                if stream == 0:
                    if p == 0:
                        for i in range(len(partners)):
                            take(hfree.at[i], chunk)
                    for i in range(2):
                        h[lax.rem(chunk, 2), i, rows(own_row(p), n2), :] = out[:, i * half:(i + 1) * half]
                ho[chunk, mine, :] = out
                if stream == 1:
                    y_copy(p, chunk).start()
                give(free.at[stream, 1, p], chunk, first_dev[col])
                give(free.at[stream, 2, p], chunk, second_dev[col])
            elif e == 4 and stream == 1:
                y_copy(p, chunk).wait()
            if e < 3:
                take(free.at[stream, e, p], chunk)
            if e < 6:
                remote(stream, e, p, chunk).start()

    for cp in qkv_copies():
        cp.start()
    for cp in x_copy(0):
        cp.start()
    for cp in wo_copies():
        cp.start()
    for chunk in range(CHUNKS):
        for p in range(parts):
            base_copy(p, chunk).start()
    pl.semaphore_wait(barrier, tp_size - 1)

    reload_wo = sorted({(s - PROLOGUE) // per_chunk for s in EVENTS[0, 0] if s >= PROLOGUE} - {0})

    @pl.loop(0, STEPS)
    def _(g):
        gm = g - PROLOGUE
        c, j = lax.div(gm, per_chunk), lax.rem(gm, per_chunk)
        computes = (gm >= 0) & (gm < CHUNKS * per_chunk)

        for it in reload_wo:
            @pl.when(gm == it * per_chunk + 1)
            def _():
                for cp in wo_copies():
                    cp.wait()

        for (stream, e), at in EVENTS.items():
            hit = functools.reduce(lambda a, b: a | b, [g == s for s in at])

            @pl.when(hit)
            def _():
                chunk = sum([(g >= s).astype(jnp.int32) for s in at[1:]])
                if stream == 2:
                    (project_qkv, attend)[e](chunk)
                else:
                    if (stream, e) == (0, 0):
                        project(chunk)
                    event(stream, e, chunk)

        @pl.when(computes & (j < gu_tiles))
        def _():
            for cp in gu_copies(c, j):
                cp.wait()

            @pl.when((j + 1 < gu_tiles) | (c + 1 < CHUNKS))
            def _():
                wraps = (j + 1 >= gu_tiles).astype(jnp.int32)
                launch(gu_copies(c + wraps, (j + 1) * (1 - wraps)))

            @pl.when(j == gu_tiles - 2)
            def _():
                launch(dn_copies(0))
            slot = lax.rem(c * gu_tiles + j, 2)
            both = times_h(lax.rem(c, 2), [wgu[slot, pl.ds(i * half, half)] for i in range(2)])
            gate, up = both[:, :GU], both[:, GU:]
            act[:, pl.ds(pl.multiple_of(j * GU, GU), GU)] = (gate * lax.logistic(gate) * up).astype(jnp.bfloat16)

            @pl.when((j == gu_tiles - 1) & (c + 2 < CHUNKS))
            def _():
                release_h()

        @pl.when(computes & (j >= gu_tiles))
        def _():
            k = j - gu_tiles
            for cp in dn_copies(k):
                cp.wait()

            @pl.when(k + 1 < dn_tiles)
            def _():
                launch(dn_copies(k + 1))
            for b in range(2):
                part[:, dn_cols(k, b)] = jnp.dot(act[...], wdb[lax.rem(k, 2), b], preferred_element_type=jnp.float32).astype(jnp.bfloat16)

            @pl.when(k + 1 == dn_tiles)
            def _():
                event(1, 0, c)
            for it in reload_wo:
                @pl.when(gm == it * per_chunk - 1)
                def _():
                    for cp in wo_copies():
                        cp.start()

    for cp in kv_copies(CHUNKS - 1):
        cp.wait()


def store_kernel(y_ref, k_ref, v_ref, y_out, k_out, v_out, buf, kv, get, put):
    pieces, rows = buf.shape[0], buf.shape[1]
    def piece(i):
        return pl.ds(i * rows, rows)
    loads = [pltpu.make_async_copy(src, kv.at[i], get.at[pieces + i]) for i, src in enumerate((k_ref, v_ref))]
    loads += [pltpu.make_async_copy(y_ref.at[piece(i)], buf.at[i], get.at[i]) for i in range(pieces)]
    stores = [pltpu.make_async_copy(kv.at[i], dst, put.at[pieces + i]) for i, dst in enumerate((k_out, v_out))]
    stores += [pltpu.make_async_copy(buf.at[i], y_out.at[piece(i)], put.at[i]) for i in range(pieces)]
    for cp in loads:
        cp.start()
    for load, store in zip(loads, stores):
        load.wait()
        store.start()
    for cp in stores:
        cp.wait()


def store(y, keys, v):
    pieces = 16
    anyspec = pl.BlockSpec(memory_space=pl.ANY)
    dma = pltpu.SemaphoreType.DMA
    return pl.pallas_call(
        store_kernel,
        out_shape=[jax.ShapeDtypeStruct(t.shape, t.dtype) for t in (y, keys, v)],
        in_specs=[anyspec] * 3,
        out_specs=[anyspec] * 3,
        scratch_shapes=[pltpu.VMEM((pieces, y.shape[0] // pieces, y.shape[1]), y.dtype), pltpu.VMEM((2,) + keys.shape, keys.dtype), dma((pieces + 2,)), dma((pieces + 2,))],
        compiler_params=pltpu.CompilerParams(vmem_limit_bytes=67043328),
    )(y, keys, v)


def solution(mesh):
    tp_size = mesh.shape['tp']

    def local_layer(tokens, seq_lens, w_q, w_k, w_v, w_o, g_q, g_k, g_attn, g_mlp, w_gate, w_up, w_down):
        prompts, seq_len, width = tokens.shape
        total, inner, q_width = prompts * seq_len, w_gate.shape[1], w_q.shape[1]
        size = total // CHUNKS
        cos, sin = rope_tables(seq_len, HEAD_DIM)
        bf, f32 = jnp.bfloat16, jnp.float32
        anyspec = pl.BlockSpec(memory_space=pl.ANY)
        vmem = pl.BlockSpec(memory_space=pltpu.VMEM)
        dma, credit = pltpu.SemaphoreType.DMA, pltpu.SemaphoreType.REGULAR
        cache_shape = jax.ShapeDtypeStruct((total, HEAD_DIM), bf)
        y, keys, v = pl.pallas_call(
            functools.partial(layer_kernel, seq_len, tp_size),
            out_shape=[jax.ShapeDtypeStruct((total, width), bf), cache_shape, cache_shape],
            in_specs=[pl.BlockSpec(memory_space=pltpu.SMEM)] + [anyspec] * 8 + [vmem] * 6,
            out_specs=[anyspec] * 3,
            scratch_shapes=[
                pltpu.VMEM((2, width, 2 * GU), bf), pltpu.VMEM((2, 2, inner, DN // 2), bf), pltpu.VMEM((2, 2, size, width // 2), bf),
                pltpu.VMEM((size, inner), bf), pltpu.VMEM((size, width), bf),
                pltpu.VMEM((2, size // 2, width), bf), pltpu.VMEM((2, size // 4, width), bf), pltpu.VMEM((2, size // 8, width), bf),
                pltpu.VMEM((size, q_width), bf), pltpu.VMEM((size, q_width + HEAD_DIM), f32), pltpu.VMEM((2, size, HEAD_DIM), bf),
                pltpu.VMEM((CHUNKS, size // 8, width), bf),
                pltpu.VMEM((CHUNKS, 8, STAT), f32), pltpu.VMEM((CHUNKS, tp_size - 1, 8, STAT), f32), pltpu.VMEM((2, 8, STAT), f32),
                dma((2, 2, 2)), dma((2, 2)), dma((width // DN, 2)), dma((3,)), dma((2,)), dma((2,)), dma((CHUNKS, 4)), dma((4,)),
                dma((CHUNKS, tp_size - 1)), dma((CHUNKS, tp_size - 1)), dma((2, CHUNKS, 6, 4)), dma((2, CHUNKS, 6, 4)),
                credit((2, 3, 4)), credit((3,)),
            ],
            compiler_params=pltpu.CompilerParams(collective_id=0, has_side_effects=True, vmem_limit_bytes=67043328),
            cost_estimate=pl.CostEstimate(flops=2 * total * width * (3 * inner + 2 * q_width + 2 * HEAD_DIM), bytes_accessed=CHUNKS * 3 * inner * width * 2, transcendentals=total * inner),
        )(seq_lens, tokens.reshape(total, width), w_q, w_k, w_v, w_o, w_gate, w_up, w_down,
          g_q, g_k, g_attn, g_mlp, jnp.asarray(cos), jnp.asarray(sin))
        y, keys, v = store(y, keys, v)
        cache = (prompts, 1, seq_len, HEAD_DIM)
        return y.reshape(prompts, seq_len, width), keys.reshape(cache), v.reshape(cache)

    return jax.shard_map(local_layer, mesh=mesh, in_specs=(P('dp', None, None), P('dp'), P(None, 'tp'), P(None, 'tp'), P(None, 'tp'), P('tp', None), P('tp'), P('tp'), P(), P(), P(None, 'tp'), P(None, 'tp'), P('tp', None)), out_specs=(P('dp', None, None), P('dp', 'tp', None, None), P('dp', 'tp', None, None)), check_vma=False)
```
